32 devices in a mesh: gy: 8 (over z, x), gx: 4 (over y, core).
Axes of the slice: x: 2, y: 2, z: 4, core: 2. Of those that a mesh axis runs over, the one named last changes fastest.
Arguments:
- ensemble: bfloat16 [32, 2, 512, 512], P(None, None, 'gy', 'gx'), may hold values from -1.1953125 to 1.1953125
- obs_cell: int32 [8, 4, 2048], P('gy', 'gx'), may hold values from 0 to 8191
- obs_level: int32 [8, 4, 2048], P('gy', 'gx'), may hold values from 0 to 1
- innovation: float32 [8, 4, 2048], P('gy', 'gx'), may hold values from -6 to 6
- obs_weight: float32 [8, 4, 2048], P('gy', 'gx'), may hold values from 0.5 to 4
Outputs:
- control: float32 [32, 2, 512, 512], P(None, None, 'gy', 'gx')
- increment: float32 [2, 512, 512], P(None, 'gy', 'gx')
The draws below stay inside these ranges and needn't reach their ends.
Inputs may be any that keep to these rules, and one draw needn't show every extreme that they name: obs_cell holds row * 128 + column of the observation within its device's block of 64 x 128 cells.
All inputs are finite; a program needn't handle non-finite values.
Results may differ from the reference program's by a relative error of at most 0.0003.
Values sent between devices are 32-bit elements; how exact they have to be, the bound alone decides.
A program may use at most 128 MiB of HBM per device.

```python
import math
import jax
import jax.numpy as jnp
from jax import lax

MEMBERS = 32
LEV = 2
SWEEPS = 4
CY = 64
CX = 128
OBS_DEV = 2048
NY = 512
NX = 512
N_GY = 8
N_GX = 4


def place_ends(result, key, smallest, high):
    dims = result.shape
    place = [jax.random.randint(jax.random.fold_in(key, axis), (), 0, dims[axis]) for axis in range(len(dims))]
    result = result.at[tuple(place)].set(smallest)
    longest = dims.index(max(dims))
    place[longest] = (place[longest] + 1) % dims[longest]
    return result.at[tuple(place)].set(high)


def block_scale(stream_key, dims, split, low, top_value):
    level = 1.0
    for axis_at, parts in split:
        draws = jax.random.uniform(jax.random.fold_in(jax.random.fold_in(stream_key, 6), axis_at), (parts,), jnp.float32, low / len(split), top_value / len(split))
        level = level * jnp.repeat(jnp.exp(draws), dims[axis_at] // parts).reshape((-1,) + (1,) * (len(dims) - 1 - axis_at))
    return level


def centred(stream_key, shape, scale, reach, cuts=(), kind=jnp.bfloat16):
    entries = scale * jax.random.normal(stream_key, shape, jnp.float32)
    if cuts:
        entries = entries * block_scale(stream_key, shape, cuts, -0.22, 0.18)
    return jnp.clip(entries, -reach, reach).astype(kind)


def setup_inputs(seed: int = 0) -> dict:
    keys = jax.random.split(jax.random.key(seed), 6)
    return {
        "ensemble": centred(keys[0], (MEMBERS, LEV, NY, NX), 0.2, 1.1953125, ((2, 8), (3, 4))),
        "obs_cell": place_ends(jax.random.randint(keys[1], (N_GY, N_GX, OBS_DEV), 0, CY * CX), jax.random.fold_in(keys[1], 1), 0, (CY * CX) - 1).astype(jnp.int32),
        "obs_level": place_ends(jax.random.randint(keys[2], (N_GY, N_GX, OBS_DEV), 0, LEV), jax.random.fold_in(keys[2], 1), 0, LEV - 1).astype(jnp.int32),
        "innovation": centred(keys[3], (N_GY, N_GX, OBS_DEV), 1.0, 6.0, ((0, 8), (1, 4)), jnp.float32),
        "obs_weight": jnp.clip(jnp.exp(math.log(4.0) - 2.0794415 * jax.random.uniform(keys[4], (N_GY, N_GX, OBS_DEV), jnp.float32) ** block_scale(keys[4], (N_GY, N_GX, OBS_DEV), ((0, 8), (1, 4)), -0.2, 0.2)), 0.5, 4.0),
    }


KAPPA = 0.2
EPS = 1e-06

def smooth_once(field):
    padded = jnp.pad(field, ((0, 0), (0, 0), (1, 1), (1, 1)))
    beside_all = padded[:, :, 2:, 1:-1] + padded[:, :, :-2, 1:-1] + padded[:, :, 1:-1, 2:] + padded[:, :, 1:-1, :-2]
    return field + KAPPA * (beside_all - 4.0 * field)

def filtered(field):
    for sweep in range(SWEEPS):
        field = smooth_once(field)
    return field

def reference(ensemble, obs_cell, obs_level, innovation, obs_weight):
    block_row = jnp.arange(N_GY, dtype=jnp.int32)[:, None, None]
    block_col = jnp.arange(N_GX, dtype=jnp.int32)[None, :, None]
    rows = block_row * CY + obs_cell // CX
    cols = block_col * CX + obs_cell % CX
    points = (obs_level * (NY * NX) + rows * NX + cols).reshape(-1).astype(jnp.int32)
    weights = obs_weight.reshape(-1)
    members = ensemble.astype(jnp.float32)

    def adjoint_obs(values):
        state = jnp.zeros((LEV * NY * NX,), jnp.float32).at[points].add(values)
        return state.reshape(LEV, NY, NX)

    def hessian(vector):
        state = lax.optimization_barrier(jnp.sum(members * filtered(vector), axis=0))
        seen = state.reshape(-1)[points]
        back = filtered(members * adjoint_obs(weights * seen)[None])
        return (vector + back, state)
    gradient = filtered(members * adjoint_obs(weights * innovation.reshape(-1))[None])
    bnorm = jnp.sqrt(jnp.sum(gradient * gradient) + EPS)
    first = gradient / bnorm
    image_one, state_one = hessian(first)
    alpha_one = jnp.sum(first * image_one)
    remain = image_one - alpha_one * first
    beta = jnp.sqrt(jnp.sum(remain * remain) + EPS)
    second = remain / beta
    image_two, state_two = hessian(second)
    alpha_two = jnp.sum(second * image_two)
    determ = alpha_one * alpha_two - beta * beta
    coef_one = bnorm * alpha_two / determ
    coef_two = -bnorm * beta / determ
    control = coef_one * first + coef_two * second
    increment = coef_one * state_one + coef_two * state_two
    return (control, increment)
```

```python
import math
import jax
import jax.numpy as jnp
from jax import lax
from jax.experimental import pallas as pl
from jax.experimental.pallas import tpu as pltpu
from jax.sharding import PartitionSpec as P

SWEEPS = 4
KAPPA = 0.2
EPS = 1e-06
D = SWEEPS
BASE = 8
LANES = 128
SIDES = [(-1, 0), (1, 0), (0, -1), (0, 1), (-1, -1), (-1, 1), (1, -1), (1, 1)]
N_, S_, W_, E_, NW, NE, SW, SE = range(8)
BACK = [S_, N_, E_, W_, SE, SW, NE, NW]
MESH = pl.DeviceIdType.MESH
f32, bf16 = jnp.float32, jnp.bfloat16


class Dims:
    def __init__(self, members, levels, rows, cols):
        self.members, self.levels, self.rows, self.cols = members, levels, rows, cols
        self.fields = members * levels
        self.halves = LANES // self.fields
        assert self.halves == 2 and cols == LANES and levels * rows == LANES
        self.r = rows // self.halves
        self.rr = self.r + 2 * D
        self.groups = (cols + 2 * D) // 8
        self.st = -(-(cols + 2 * D) // 16) * 16
        self.size = BASE + self.rr * self.st + 8


def peer(dy, dx):
    ny, nx = lax.axis_size("gy"), lax.axis_size("gx")
    return {"gy": lax.rem(lax.axis_index("gy") + dy + ny, ny), "gx": lax.rem(lax.axis_index("gx") + dx + nx, nx)}


def meet_signal():
    bar = pltpu.get_barrier_semaphore()
    for dy, dx in SIDES:
        pl.semaphore_signal(bar, inc=1, device_id=peer(dy, dx), device_id_type=MESH)
    for axis in ("gx", "gy"):
        n, me = lax.axis_size(axis), lax.axis_index(axis)
        for k in range(1, n):
            pl.semaphore_signal(bar, inc=1, device_id={axis: lax.rem(me + k, n)}, device_id_type=MESH)


def meet_wait():
    total = len(SIDES) + lax.axis_size("gx") + lax.axis_size("gy") - 2
    pl.semaphore_wait(pltpu.get_barrier_semaphore(), total)


def send(n, src, dst, ssem, rsem):
    dy, dx = SIDES[n]
    c = pltpu.make_async_remote_copy(src_ref=src, dst_ref=dst, send_sem=ssem.at[n], recv_sem=rsem.at[n],
                                     device_id=peer(dy, dx), device_id_type=MESH)
    c.start()
    return c


def lane_iota(rows):
    return lax.broadcasted_iota(jnp.int32, (rows, LANES), 1)


def flip(x):
    return pltpu.roll(x, LANES // 2, 1)


def scatter(d, cell_ref, level_ref, inn_ref, wt_ref, go, do):
    cell = cell_ref[...]
    row = level_ref[...] * d.rows + cell // d.cols
    col = cell % d.cols
    n = cell.shape[1]
    hot = jnp.where(lax.broadcasted_iota(jnp.int32, (d.levels * d.rows, n), 0) == row, 1.0, 0.0).astype(bf16)
    at = lax.broadcasted_iota(jnp.int32, (d.cols, n), 0) == col
    wt = wt_ref[...]
    for ref, v in ((go, wt * inn_ref[...]), (do, wt)):
        hi = v.astype(bf16).astype(f32)
        total = None
        for part in (hi, v - hi):
            sel = jnp.where(at, part, 0.0).astype(bf16)
            term = lax.dot_general(sel, hot, (((1,), (1,)), ((), ())), preferred_element_type=f32)
            total = term if total is None else total + term
        ref[D:D + d.cols, :] = total
        ref[0:D, :] = jnp.zeros((D, LANES), f32)
        ref[D + d.cols:d.st, :] = jnp.zeros((d.st - D - d.cols, LANES), f32)


def row_masks(d, rows):
    rowl = lane_iota(rows) % d.rows
    return rowl < D, rowl >= d.rows - D, (rowl >= d.r - D) & (rowl < d.r + D)


def exchange_buffers(n):
    v = lambda *s: pltpu.VMEM((n,) + s, f32)
    one = [v(3, 8, LANES)] * 2 + [v(2, 8, LANES)] * 2 + [v(8, LANES)] * 4
    dma = pltpu.SemaphoreType.DMA
    return one + one + [dma((8,)), dma((8,))]


def exchange(d, pairs, bufs):
    out, land, ssem, rsem = bufs[:8], bufs[8:16], bufs[16], bufs[17]
    lo, hi, mid = row_masks(d, 8)
    last = d.groups - 1
    at = lambda g: slice(g * 8, g * 8 + 8)
    for a, (yo, yr) in enumerate(pairs):
        packs = [[None] * 3, [None] * 3]
        for g in range(d.groups):
            own, ring = yo[at(g), :], yr[at(g), :]
            own = own + jnp.where(mid, ring, 0.0)
            yo[at(g), :] = own
            for k in range(2):
                v = jnp.where(lo, own if k == 0 else ring, jnp.where(hi, ring if k == 0 else own, 0.0))
                if g == 0:
                    out[NW + 2 * k][a] = v
                if g == last:
                    out[NE + 2 * k][a] = v
                v = pltpu.roll(v, D + 8 * (g % 8), 1)
                packs[k][g // 8] = v if packs[k][g // 8] is None else packs[k][g // 8] + v
            if g == 0 or g == last:
                m = out[W_ if g == 0 else E_]
                m[a, 0] = own
                m[a, 1] = ring
        for k in range(2):
            for j in range(3):
                out[k][a, j] = packs[k][j]
    copies = [send(n, out[n], land[BACK[n]], ssem, rsem) for n in (N_, S_, W_, E_, NW, NE, SW, SE)]
    for c in copies:
        c.wait_recv()
    for a, (yo, yr) in enumerate(pairs):
        for g in range(d.groups):
            own, ring = yo[at(g), :], yr[at(g), :]
            shift = (LANES - D - 8 * (g % 8)) % LANES
            north = pltpu.roll(land[N_][a, g // 8], shift, 1)
            south = pltpu.roll(land[S_][a, g // 8], shift, 1)
            if g == 0:
                north, south = north + land[NW][a], south + land[SW][a]
            if g == last:
                north, south = north + land[NE][a], south + land[SE][a]
            if g == 0 or g == last:
                m = land[W_ if g == 0 else E_]
                own, ring = own + m[a, 0], ring + m[a, 1]
            own = own + jnp.where(lo, north, jnp.where(hi, south, 0.0))
            ring = ring + jnp.where(hi, north, jnp.where(lo, south, 0.0))
            yo[at(g), :] = own
            yr[at(g), :] = jnp.where(mid, own, ring)
    return copies


def build_selectors(d, sel, bsel):
    def code(x_iota, l_iota):
        level = x_iota // d.rows
        half = l_iota // d.fields
        base = lax.rem(lax.rem(x_iota, d.rows) - d.r * half + d.rows, d.rows)
        return jnp.where(lax.rem(l_iota, d.levels) == level, base, -1)

    a = lax.broadcasted_iota(jnp.int32, (LANES, LANES), 0)
    b = lax.broadcasted_iota(jnp.int32, (LANES, LANES), 1)
    for_sel, for_bsel = code(a, b), code(b, a)

    def fill(q, x):
        for s in range(2):
            i = q * 2 + s
            want = lax.rem(i - D + d.rows, d.rows)
            one = jnp.where(for_sel == want, 1.0, 0.0).astype(bf16)
            two = jnp.where(for_bsel == want, 1.0, 0.0).astype(bf16)
            for k in range(2):
                sel[q, k * LANES:(k + 1) * LANES, s * LANES:(s + 1) * LANES] = one
                bsel[pl.ds(pl.multiple_of(i * 256 + k * LANES, LANES), LANES), :] = two
        return x

    lax.fori_loop(0, d.rr // 2, fill, 0)


def split(x):
    hi = x.astype(bf16)
    return hi, (x - hi.astype(f32)).astype(bf16)


def expand(d, go, gr, sel, et, u):
    def wide(ref):
        hi, lo = split(ref[...])
        return jnp.concatenate([hi, lo], axis=1)

    own, ring = wide(go), wide(gr)
    pairs = d.rr // 2
    edge = D // 2
    for q in range(pairs):
        x = ring if q < edge or q >= pairs - edge else own
        g2 = jnp.dot(x, sel[q], preferred_element_type=f32)
        for s in range(2):
            at = BASE + (2 * q + s) * d.st
            n = d.groups * 8
            u[at:at + n, :] = et[at:at + n, :] * g2[0:n, s * LANES:(s + 1) * LANES]


def stencil(d, src, p, lo, hi, use):
    def ld(r, o):
        return src[pl.ds(p + (BASE + (r + D) * d.st + o), 8), :]

    n, c = ld(lo - 1, 0), ld(lo, 0)
    for r in range(lo, hi):
        s = ld(r + 1, 0)
        use(r, (n + s) + (c + (ld(r, -1) + ld(r, 1))))
        n, c = c, s


def sweep(d, src, dst, ext, masks):
    cm, rt, rb = masks

    def body(g, x):
        p = pl.multiple_of(g * 8, 8)
        m = cm[pl.ds(p, 8), :]
        mt, mb = m * rt[...], m * rb[...]

        def use(r, v):
            dst[pl.ds(p + (BASE + (r + D) * d.st), 8), :] = v * (mt if r < 0 else mb if r >= d.r else m)

        stencil(d, src, p, -ext, d.r + ext, use)
        return x

    lax.fori_loop(0, d.groups, body, 0)


def half_filter(d, src, bufs, pad, po, masks):
    a1, a2, a3 = bufs
    sweep(d, src, a1, 3, masks)
    sweep(d, a1, a2, 2, masks)
    sweep(d, a2, a3, 1, masks)

    def body(g, x):
        p = g * 8 + D

        def use(r, v):
            pad[pl.ds(p + (BASE + (r + D) * d.st), 8), :] = v
            po[r, pl.ds(pl.multiple_of(g * 8, 8), 8), :] = v

        stencil(d, a3, p, 0, d.r, use)
        return x

    lax.fori_loop(0, d.cols // 8, body, 0)


def back_filter(d, pad, bufs, et, lhs, masks):
    b1, b2, b3 = bufs
    sweep(d, pad, b1, 1, masks)
    sweep(d, b1, b2, 2, masks)
    sweep(d, b2, b3, 3, masks)
    zero = jnp.zeros((8, LANES), f32)

    def pair(p, q, both):
        def ld(r, o):
            return b3[pl.ds(p + (BASE + (r + D) * d.st + o), 8), :]

        n = [None, None]
        c = [ld(-D, 0), ld(-D, 8) if both else None]
        for r in range(-D, d.r + D):
            ts = []
            for k in range(2 if both else 1):
                o = 8 * k
                v = c[k] + (ld(r, o - 1) + ld(r, o + 1))
                s = None
                if r < d.r + D - 1:
                    s = ld(r + 1, o)
                    v = v + s
                if r > -D:
                    v = v + n[k]
                n[k], c[k] = c[k], s
                ts.append(v * et[pl.ds(p + (BASE + (r + D) * d.st + o), 8), :])
            if not both:
                ts.append(zero)
            hi, lo = split(jnp.concatenate(ts, axis=0))
            at = (r + D) * 2 * LANES
            lhs[pl.ds(q, 16), at:at + LANES] = hi
            lhs[pl.ds(q, 16), at + LANES:at + 2 * LANES] = lo

    def body(g, x):
        p = pl.multiple_of(g * 16, 16)
        pair(p, p, True)
        return x

    lax.fori_loop(0, d.groups // 2, body, 0)
    pair(d.groups // 2 * 16, d.groups // 2 * 16, False)


def reduce_members(d, lhs, bsel, yo, yr):
    k0, k1, k2 = D * 2 * LANES, (D + d.r) * 2 * LANES, d.rr * 2 * LANES
    scale = KAPPA ** (2 * SWEEPS)
    dot = lambda a, b: jnp.dot(lhs[:, a:b], bsel[a:b, :], preferred_element_type=f32)
    yo[...] = dot(k0, k1) * scale
    yr[...] = (dot(0, k0) + dot(k1, k2)) * scale


def all_sum(x_ref, o_ref, mid_ref, ra_ref, rb_ref, sa, qa, sb, qb):
    nx, ny = lax.axis_size("gx"), lax.axis_size("gy")
    mx, my = lax.axis_index("gx"), lax.axis_index("gy")

    def stage(axis, n, me, src, land, ssem, rsem):
        copies = []
        for k in range(1, n):
            copies.append(pltpu.make_async_remote_copy(
                src_ref=src, dst_ref=land.at[k - 1], send_sem=ssem.at[k - 1], recv_sem=rsem.at[k - 1],
                device_id={axis: lax.rem(me + k, n)}, device_id_type=MESH))
            copies[-1].start()
        for c in copies:
            c.wait_recv()
        total = src[...]
        for k in range(n - 1):
            total = total + land[k]
        return copies, total

    ca, total = stage("gx", nx, mx, x_ref, ra_ref, sa, qa)
    mid_ref[...] = total
    cb, total = stage("gy", ny, my, mid_ref, rb_ref, sb, qb)
    o_ref[...] = total
    for c in ca + cb:
        c.wait_send()


def ens_send_rows(d, et, hn, hs):
    lane = lane_iota(d.cols)
    low = lane < LANES // 2
    at = lambda r: et[BASE + (r + D) * d.st + D:BASE + (r + D) * d.st + D + d.cols, :]
    for i in range(2):
        hn[i] = jnp.where(low, at(i), flip(at(i + 2)))
        hs[i] = jnp.where(low, flip(at(d.r - 2 + i)), at(d.r - 4 + i))


def main_kernel(d, ens, cell, level, inn, wt, p0_out, p1_out, y0_out, y1_out, m_out, *refs):
    refs = list(refs)
    take = lambda n: [refs.pop(0) for _ in range(n)]
    ec, et, u, a1, a2, a3, pad, b1, b2, b3 = take(10)
    sel, bsel, lhs, po0, po1 = take(5)
    cm, rt, rb = masks = take(3)
    hn, hs, hw, he, ln, ls, lw, le, lnw, lne, lsw, lse, esem, rsem = take(14)
    go, gr, do, dr, g1o, g1r, y0o, y0r, y1o, y1r = take(10)
    ex0, ex1, ex2 = take(18), take(18), take(18)
    x_ref, mid_ref, ra_ref, rb_ref, sa, qa, sb, qb = take(8)
    osem = refs.pop(0)
    es = d.rows + 1
    gy, gx = lax.axis_index("gy"), lax.axis_index("gx")
    ny, nx = lax.axis_size("gy"), lax.axis_size("gx")
    flag = lambda b: jnp.where(b, 1.0, 0.0).astype(f32)
    hasn, hass, hasw, hase = flag(gy > 0), flag(gy < ny - 1), flag(gx > 0), flag(gx < nx - 1)

    meet_signal()

    def convert(k, x):
        for l in range(d.levels):
            ec[pl.ds((k * d.levels + l) * es, d.rows), :] = ens[k, l].astype(f32)
        return x

    lax.fori_loop(0, d.members, convert, 0)

    def transpose_row(r):
        parts = []
        for h in range(d.halves):
            for f in range(0, d.fields, 8):
                parts.append(ec[pl.ds(f * es + h * d.r + r, 8, stride=es), :])
        et[pl.ds(BASE + (r + D) * d.st + D, d.cols), :] = jnp.concatenate(parts, axis=0).T

    for r in list(range(4)) + list(range(d.r - 4, d.r)):
        transpose_row(r)
    ens_send_rows(d, et, hn, hs)
    meet_wait()
    ecopies = [send(N_, hn, ls, esem, rsem), send(S_, hs, ln, esem, rsem)]

    def more(q, x):
        for s in range(4):
            transpose_row(q * 4 + s)
        return x

    lax.fori_loop(1, d.r // 4 - 1, more, 0)
    for r in range(d.r):
        at = BASE + (r + D) * d.st + D
        hw[r * 4:r * 4 + 4, :] = et[at:at + 4, :]
        he[r * 4:r * 4 + 4, :] = et[at + d.cols - 4:at + d.cols, :]
    n4 = d.r * 4
    ecopies += [send(W_, hw, le, esem, rsem), send(E_, he, lw, esem, rsem),
                send(NW, hw.at[0:16], lse, esem, rsem), send(NE, he.at[0:16], lsw, esem, rsem),
                send(SW, hw.at[n4 - 16:n4], lne, esem, rsem), send(SE, he.at[n4 - 16:n4], lnw, esem, rsem)]

    scatter(d, cell, level, inn, wt, go, do)
    gr[...] = jnp.zeros_like(gr)
    dr[...] = jnp.zeros_like(dr)
    gcopies = exchange(d, [(go, gr), (do, dr)], ex0)
    build_selectors(d, sel, bsel)
    p = lax.broadcasted_iota(jnp.int32, (d.groups * 8, LANES), 0)
    cm[...] = jnp.where(p < D, hasw, jnp.where(p >= D + d.cols, hase, 1.0))
    low8 = lane_iota(8) < LANES // 2
    rt[...] = jnp.where(low8, hasn, 1.0)
    rb[...] = jnp.where(low8, 1.0, hass)

    zero = lambda n: jnp.zeros((n, LANES), f32)
    for ref, ext in ((pad, 0), (b1, 1), (b2, 2), (b3, 3)):
        for r in range(-min(ext + 2, D), d.r + min(ext + 2, D)):
            at = BASE + (r + D) * d.st
            if r < -ext or r >= d.r + ext:
                ref[at:at + d.st, :] = zero(d.st)
            else:
                ref[at + d.groups * 8:at + d.st, :] = zero(d.st - d.groups * 8)
                if ext == 0:
                    ref[at:at + D, :] = zero(D)
                    ref[at + D + d.cols:at + d.groups * 8, :] = zero(D)
        ref[0:BASE, :] = zero(BASE)
        ref[BASE + d.rr * d.st:d.size, :] = zero(8)

    for c in ecopies:
        c.wait_recv()
    low = lane_iota(d.cols) < LANES // 2
    row_at = lambda r: BASE + (r + D) * d.st
    own = lambda r: et[row_at(r) + D:row_at(r) + D + d.cols, :]
    for j in range(D):
        south = ls[j % 2] * hass
        north = ln[j % 2] * hasn
        if j < 2:
            sv = flip(jnp.where(low, south, own(j)))
            nv = flip(jnp.where(low, own(d.r - 4 + j), north))
        else:
            sv = jnp.where(low, flip(own(j)), south)
            nv = jnp.where(low, north, flip(own(d.r - 4 + j)))
        et[row_at(d.r + j) + D:row_at(d.r + j) + D + d.cols, :] = sv
        et[row_at(j - D) + D:row_at(j - D) + D + d.cols, :] = nv
    low16 = lane_iota(16) < LANES // 2
    for land, north, south, ok, off in ((lw, lnw, lsw, hasw, 0), (le, lne, lse, hase, D + d.cols)):
        for r in range(d.r):
            et[row_at(r) + off:row_at(r) + off + 4, :] = land[r * 4:r * 4 + 4, :] * ok
        nv = flip(jnp.where(low16, land[n4 - 16:n4, :], north[...] * hasn)) * ok
        sv = flip(jnp.where(low16, south[...] * hass, land[0:16, :])) * ok
        for j in range(D):
            et[row_at(j - D) + off:row_at(j - D) + off + 4, :] = nv[j * 4:j * 4 + 4, :]
            et[row_at(d.r + j) + off:row_at(d.r + j) + off + 4, :] = sv[j * 4:j * 4 + 4, :]

    def g_step(g_o, g_r, po, out, n, yo, yr):
        expand(d, g_o, g_r, sel, et, u)
        half_filter(d, u, (a1, a2, a3), pad, po, masks)
        copy = pltpu.make_async_copy(po, out, osem.at[n])
        copy.start()
        back_filter(d, pad, (b1, b2, b3), et, lhs, masks)
        reduce_members(d, lhs, bsel, yo, yr)
        return copy

    o0 = g_step(go, gr, po0, p0_out, 0, y0o, y0r)
    ycopies = exchange(d, [(y0o, y0r)], ex1)
    g1o[...] = do[...] * y0o[...]
    g1r[...] = dr[...] * y0r[...]
    o1 = g_step(g1o, g1r, po1, p1_out, 1, y1o, y1r)
    zcopies = exchange(d, [(y1o, y1r)], ex2)
    inner = slice(D, D + d.cols)
    y0, y1, g0, g1, dd = y0o[inner, :], y1o[inner, :], go[inner, :], g1o[inner, :], do[inner, :]
    x_ref[...] = jnp.zeros_like(x_ref)
    for k, v in enumerate((g0 * y0, g1 * y0, g1 * y1, dd * y1 * y1)):
        x_ref[k:k + 1, :] = jnp.sum(v, axis=0, keepdims=True)
    y0_out[...] = y0
    y1_out[...] = y1
    all_sum(x_ref, m_out, mid_ref, ra_ref, rb_ref, sa, qa, sb, qb)
    for c in ecopies + gcopies + ycopies + zcopies:
        c.wait_send()
    o0.wait()
    o1.wait()


def final_kernel(d, p0, p1, y0, y1, m_ref, c_ref, inc_ref):
    m = jnp.sum(m_ref[...], axis=1, keepdims=True)
    m = [m[k:k + 1] for k in range(4)]
    bn2 = m[0] + EPS
    c = (EPS - m[1]) / bn2
    alpha1 = (m[0] + m[1]) / bn2
    r2 = jnp.maximum((c * c * m[0] + 2.0 * c * m[1] + m[2]) / bn2, 0.0)
    rho = (c * c * m[1] + 2.0 * c * m[2] + m[3]) / bn2
    b2 = r2 + EPS
    alpha2 = (r2 + rho) / b2
    det = alpha1 * alpha2 - b2
    ca, cb = (alpha2 - c) / det, -1.0 / det
    wide = lambda v: jnp.broadcast_to(v, (LANES, LANES))
    scale = KAPPA ** SWEEPS
    sa, sb = wide(ca * scale), wide(cb * scale)
    inc = (wide(ca) * y0[...] + wide(cb) * y1[...]).T
    for l in range(d.levels):
        inc_ref[l] = inc[l * d.rows:(l + 1) * d.rows]
    step = p0.shape[0]
    for r in range(step):
        v = (sa * p0[r] + sb * p1[r]).T
        for h in range(d.halves):
            for f in range(0, d.fields, 8):
                at = h * d.fields + f
                c_ref[pl.ds((f * d.halves + h) * step + r, 8, stride=d.halves * step), :] = v[at:at + 8]


def on_device(ensemble, obs_cell, obs_level, innovation, obs_weight):
    members, levels, rows, cols = ensemble.shape
    d = Dims(members, levels, rows, cols)
    nx, ny = lax.axis_size("gx"), lax.axis_size("gy")
    vm = pl.BlockSpec(memory_space=pltpu.VMEM)
    hbm = pl.BlockSpec(memory_space=pltpu.HBM)
    dma = pltpu.SemaphoreType.DMA
    v = lambda *s: pltpu.VMEM(s, f32)
    flat = lambda a: a.reshape(1, -1)
    shape = lambda *s: jax.ShapeDtypeStruct(s, f32)
    scratch = [v(d.fields * (rows + 1), LANES)] + [v(d.size, LANES)] * 9
    scratch += [pltpu.VMEM((d.rr // 2, 256, 256), bf16), pltpu.VMEM((d.rr * 256, LANES), bf16),
                pltpu.VMEM((d.st, d.rr * 256), bf16), v(d.r, cols, LANES), v(d.r, cols, LANES)]
    scratch += [v(d.groups * 8, LANES), v(8, LANES), v(8, LANES)]
    side = d.r * 4
    scratch += [v(2, cols, LANES), v(2, cols, LANES), v(side, LANES), v(side, LANES)] * 2
    scratch += [v(16, LANES)] * 4 + [dma((8,)), dma((8,))]
    scratch += [v(d.st, LANES)] * 10
    scratch += exchange_buffers(2) + exchange_buffers(1) + exchange_buffers(1)
    scratch += [v(8, LANES), v(8, LANES), v(nx - 1, 8, LANES), v(ny - 1, 8, LANES), dma((nx - 1,)), dma((nx - 1,)),
                dma((ny - 1,)), dma((ny - 1,)), dma((2,))]

    def main_entry(*refs):
        main_kernel(d, *refs)

    def final_entry(*refs):
        final_kernel(d, *refs)

    p0, p1, y0, y1, m = pl.pallas_call(
        main_entry,
        out_shape=(shape(d.r, cols, LANES), shape(d.r, cols, LANES), shape(cols, LANES), shape(cols, LANES), shape(8, LANES)),
        in_specs=[vm] * 5,
        out_specs=(hbm, hbm, vm, vm, vm),
        scratch_shapes=scratch,
        compiler_params=pltpu.CompilerParams(collective_id=0, has_side_effects=True, vmem_limit_bytes=64000000),
    )(ensemble, flat(obs_cell), flat(obs_level), flat(innovation), flat(obs_weight))
    step = 8
    block = d.fields * d.halves * step
    full = lambda *s: pl.BlockSpec(s, lambda i: (0,) * len(s))
    out4 = (d.r // step, block, LANES)

    def final_grid(p0, p1, y0, y1, m, c_ref, inc_ref, buf, sem):
        i = pl.program_id(0)
        steps = pl.num_programs(0)
        slot = lax.rem(i, 2)

        def copy(j, k):
            return pltpu.make_async_copy(
                buf.at[k].reshape(d.fields * d.halves, step, LANES),
                c_ref.at[:, pl.ds(pl.multiple_of(j * step, step), step), :], sem.at[k])

        @pl.when(i >= 2)
        def _():
            copy(i - 2, slot).wait()

        final_kernel(d, p0, p1, y0, y1, m, buf.at[slot], inc_ref)
        copy(i, slot).start()

        @pl.when(i == steps - 1)
        def _():
            copy(i - 1, 1 - slot).wait()
            copy(i, slot).wait()

    control, increment = pl.pallas_call(
        final_grid,
        grid=(d.r // step,),
        out_shape=(shape(d.fields * d.halves, d.r, LANES), shape(levels, rows, cols)),
        in_specs=[pl.BlockSpec((step, cols, LANES), lambda i: (i, 0, 0))] * 2 + [full(cols, LANES)] * 2 + [full(8, LANES)],
        out_specs=(hbm, full(levels, rows, cols)),
        scratch_shapes=[v(2, block, LANES), dma((2,))],
        compiler_params=pltpu.CompilerParams(vmem_limit_bytes=20000000),
    )(p0, p1, y0, y1, m)
    return (control.reshape(members, levels, rows, cols), increment)


def solution(mesh):
    return jax.shard_map(
        on_device,
        mesh=mesh,
        in_specs=(
            P(None, None, "gy", "gx"),
            P("gy", "gx", None),
            P("gy", "gx", None),
            P("gy", "gx", None),
            P("gy", "gx", None),
        ),
        out_specs=(P(None, None, "gy", "gx"), P(None, "gy", "gx")),
        check_vma=False,
    )
```

```python
import math
import jax
import jax.numpy as jnp
from jax import lax
from jax.experimental import pallas as pl
from jax.experimental.pallas import tpu as pltpu
from jax.sharding import PartitionSpec as P

SWEEPS = 4
KAPPA = 0.2
EPS = 1e-06
D = SWEEPS
BASE = 8
LANES = 128
SIDES = [(-1, 0), (1, 0), (0, -1), (0, 1), (-1, -1), (-1, 1), (1, -1), (1, 1)]
N_, S_, W_, E_, NW, NE, SW, SE = range(8)
BACK = [S_, N_, E_, W_, SE, SW, NE, NW]
MESH = pl.DeviceIdType.MESH
f32, bf16 = jnp.float32, jnp.bfloat16


class Dims:
    def __init__(self, members, levels, rows, cols):
        self.members, self.levels, self.rows, self.cols = members, levels, rows, cols
        self.fields = members * levels
        self.halves = LANES // self.fields
        assert self.halves == 2 and cols == LANES and levels * rows == LANES
        self.r = rows // self.halves
        self.rr = self.r + 2 * D
        self.groups = (cols + 2 * D) // 8
        self.st = -(-(cols + 2 * D) // 16) * 16
        self.size = BASE + self.rr * self.st + 8


def peer(dy, dx):
    ny, nx = lax.axis_size("gy"), lax.axis_size("gx")
    return {"gy": lax.rem(lax.axis_index("gy") + dy + ny, ny), "gx": lax.rem(lax.axis_index("gx") + dx + nx, nx)}


def others():
    ny, nx = lax.axis_size("gy"), lax.axis_size("gx")
    return [(dy, dx) for dy in range(ny) for dx in range(nx) if dy or dx]


def meet_signal():
    bar = pltpu.get_barrier_semaphore()
    for dy, dx in others():
        pl.semaphore_signal(bar, inc=1, device_id=peer(dy, dx), device_id_type=MESH)


def meet_wait():
    pl.semaphore_wait(pltpu.get_barrier_semaphore(), len(others()))


def present(n):
    dy, dx = SIDES[n]
    gy, gx = lax.axis_index("gy") + dy, lax.axis_index("gx") + dx
    ok = None
    for d, i, axis in ((dy, gy, "gy"), (dx, gx, "gx")):
        if d:
            t = (i >= 0) if d < 0 else (i < lax.axis_size(axis))
            ok = t if ok is None else ok & t
    return ok


class Side:
    def __init__(self, n, src, dst, ssem, rsem):
        dy, dx = SIDES[n]
        self.n = n
        self.copy = pltpu.make_async_remote_copy(src_ref=src, dst_ref=dst, send_sem=ssem.at[n], recv_sem=rsem.at[n],
                                                 device_id=peer(dy, dx), device_id_type=MESH)
        pl.when(present(n))(self.copy.start)

    def wait_recv(self):
        pl.when(present(BACK[self.n]))(self.copy.wait_recv)

    def wait_send(self):
        pl.when(present(self.n))(self.copy.wait_send)


def clear_absent(n, refs):
    @pl.when(jnp.logical_not(present(n)))
    def _():
        for ref in refs:
            ref[...] = jnp.zeros_like(ref)


def lane_iota(rows):
    return lax.broadcasted_iota(jnp.int32, (rows, LANES), 1)


def flip(x):
    return pltpu.roll(x, LANES // 2, 1)


def scatter(d, cell_ref, level_ref, inn_ref, wt_ref, go, do):
    cell = cell_ref[...]
    row = level_ref[...] * d.rows + cell // d.cols
    col = cell % d.cols
    n = cell.shape[1]
    hot = jnp.where(lax.broadcasted_iota(jnp.int32, (d.levels * d.rows, n), 0) == row, 1.0, 0.0).astype(bf16)
    at = lax.broadcasted_iota(jnp.int32, (d.cols, n), 0) == col
    wt = wt_ref[...]
    for ref, v in ((go, wt * inn_ref[...]), (do, wt)):
        hi = v.astype(bf16).astype(f32)
        total = None
        for part in (hi, v - hi):
            sel = jnp.where(at, part, 0.0).astype(bf16)
            term = lax.dot_general(sel, hot, (((1,), (1,)), ((), ())), preferred_element_type=f32)
            total = term if total is None else total + term
        ref[D:D + d.cols, :] = total
        ref[0:D, :] = jnp.zeros((D, LANES), f32)
        ref[D + d.cols:d.st, :] = jnp.zeros((d.st - D - d.cols, LANES), f32)


def row_masks(d, rows):
    rowl = lane_iota(rows) % d.rows
    return rowl < D, rowl >= d.rows - D, (rowl >= d.r - D) & (rowl < d.r + D)


def exchange_buffers(n):
    v = lambda *s: pltpu.VMEM((n,) + s, f32)
    one = [v(3, 8, LANES)] * 2 + [v(2, 8, LANES)] * 2 + [v(8, LANES)] * 4
    dma = pltpu.SemaphoreType.DMA
    return one + one + [dma((8,)), dma((8,))]


def exchange(d, pairs, bufs):
    out, land, ssem, rsem = bufs[:8], bufs[8:16], bufs[16], bufs[17]
    lo, hi, mid = row_masks(d, 8)
    last = d.groups - 1
    at = lambda g: slice(g * 8, g * 8 + 8)
    for a, (yo, yr) in enumerate(pairs):
        packs = [[None] * 3, [None] * 3]
        for g in range(d.groups):
            own, ring = yo[at(g), :], yr[at(g), :]
            own = own + jnp.where(mid, ring, 0.0)
            yo[at(g), :] = own
            for k in range(2):
                v = jnp.where(lo, own if k == 0 else ring, jnp.where(hi, ring if k == 0 else own, 0.0))
                if g == 0:
                    out[NW + 2 * k][a] = v
                if g == last:
                    out[NE + 2 * k][a] = v
                v = pltpu.roll(v, D + 8 * (g % 8), 1)
                packs[k][g // 8] = v if packs[k][g // 8] is None else packs[k][g // 8] + v
            if g == 0 or g == last:
                m = out[W_ if g == 0 else E_]
                m[a, 0] = own
                m[a, 1] = ring
        for k in range(2):
            for j in range(3):
                out[k][a, j] = packs[k][j]
    copies = [Side(n, out[n], land[BACK[n]], ssem, rsem) for n in (N_, S_, W_, E_, NW, NE, SW, SE)]
    for c in copies:
        c.wait_recv()
    for a, (yo, yr) in enumerate(pairs):
        for g in range(d.groups):
            own, ring = yo[at(g), :], yr[at(g), :]
            shift = (LANES - D - 8 * (g % 8)) % LANES
            north = pltpu.roll(land[N_][a, g // 8], shift, 1)
            south = pltpu.roll(land[S_][a, g // 8], shift, 1)
            if g == 0:
                north, south = north + land[NW][a], south + land[SW][a]
            if g == last:
                north, south = north + land[NE][a], south + land[SE][a]
            if g == 0 or g == last:
                m = land[W_ if g == 0 else E_]
                own, ring = own + m[a, 0], ring + m[a, 1]
            own = own + jnp.where(lo, north, jnp.where(hi, south, 0.0))
            ring = ring + jnp.where(hi, north, jnp.where(lo, south, 0.0))
            yo[at(g), :] = own
            yr[at(g), :] = jnp.where(mid, own, ring)
    return copies


def build_selectors(d, sel, bsel):
    def code(x_iota, l_iota):
        level = x_iota // d.rows
        half = l_iota // d.fields
        base = lax.rem(lax.rem(x_iota, d.rows) - d.r * half + d.rows, d.rows)
        return jnp.where(lax.rem(l_iota, d.levels) == level, base, -1)

    a = lax.broadcasted_iota(jnp.int32, (LANES, LANES), 0)
    b = lax.broadcasted_iota(jnp.int32, (LANES, LANES), 1)
    for_sel, for_bsel = code(a, b), code(b, a)

    def fill(q, x):
        for s in range(2):
            i = q * 2 + s
            want = lax.rem(i - D + d.rows, d.rows)
            one = jnp.where(for_sel == want, 1.0, 0.0).astype(bf16)
            two = jnp.where(for_bsel == want, 1.0, 0.0).astype(bf16)
            for k in range(2):
                sel[q, k * LANES:(k + 1) * LANES, s * LANES:(s + 1) * LANES] = one
                bsel[pl.ds(pl.multiple_of(i * 256 + k * LANES, LANES), LANES), :] = two
        return x

    lax.fori_loop(0, d.rr // 2, fill, 0)


def split(x):
    hi = x.astype(bf16)
    return hi, (x - hi.astype(f32)).astype(bf16)


def expand(d, go, gr, sel, et, u):
    def wide(ref):
        hi, lo = split(ref[...])
        return jnp.concatenate([hi, lo], axis=1)

    own, ring = wide(go), wide(gr)
    pairs = d.rr // 2
    edge = D // 2
    for q in range(pairs):
        x = ring if q < edge or q >= pairs - edge else own
        g2 = jnp.dot(x, sel[q], preferred_element_type=f32)
        for s in range(2):
            at = BASE + (2 * q + s) * d.st
            n = d.groups * 8
            u[at:at + n, :] = et[at:at + n, :] * g2[0:n, s * LANES:(s + 1) * LANES]


def stencil(d, src, p, lo, hi, use):
    def ld(r, o):
        return src[pl.ds(p + (BASE + (r + D) * d.st + o), 8), :]

    n, c = ld(lo - 1, 0), ld(lo, 0)
    for r in range(lo, hi):
        s = ld(r + 1, 0)
        use(r, (n + s) + (c + (ld(r, -1) + ld(r, 1))))
        n, c = c, s


def sweep(d, src, dst, ext, masks):
    cm, rt, rb = masks

    def body(g, x):
        p = pl.multiple_of(g * 8, 8)
        m = cm[pl.ds(p, 8), :]
        mt, mb = m * rt[...], m * rb[...]

        def use(r, v):
            dst[pl.ds(p + (BASE + (r + D) * d.st), 8), :] = v * (mt if r < 0 else mb if r >= d.r else m)

        stencil(d, src, p, -ext, d.r + ext, use)
        return x

    lax.fori_loop(0, d.groups, body, 0)


def half_filter(d, src, bufs, pad, po, masks):
    a1, a2, a3 = bufs
    sweep(d, src, a1, 3, masks)
    sweep(d, a1, a2, 2, masks)
    sweep(d, a2, a3, 1, masks)

    def body(g, x):
        p = g * 8 + D

        def use(r, v):
            pad[pl.ds(p + (BASE + (r + D) * d.st), 8), :] = v
            po[r, pl.ds(pl.multiple_of(g * 8, 8), 8), :] = v

        stencil(d, a3, p, 0, d.r, use)
        return x

    lax.fori_loop(0, d.cols // 8, body, 0)


def back_filter(d, pad, bufs, et, lhs, masks):
    b1, b2, b3 = bufs
    sweep(d, pad, b1, 1, masks)
    sweep(d, b1, b2, 2, masks)
    sweep(d, b2, b3, 3, masks)
    zero = jnp.zeros((8, LANES), f32)

    def pair(p, q, both):
        def ld(r, o):
            return b3[pl.ds(p + (BASE + (r + D) * d.st + o), 8), :]

        n = [None, None]
        c = [ld(-D, 0), ld(-D, 8) if both else None]
        for r in range(-D, d.r + D):
            ts = []
            for k in range(2 if both else 1):
                o = 8 * k
                v = c[k] + (ld(r, o - 1) + ld(r, o + 1))
                s = None
                if r < d.r + D - 1:
                    s = ld(r + 1, o)
                    v = v + s
                if r > -D:
                    v = v + n[k]
                n[k], c[k] = c[k], s
                ts.append(v * et[pl.ds(p + (BASE + (r + D) * d.st + o), 8), :])
            if not both:
                ts.append(zero)
            hi, lo = split(jnp.concatenate(ts, axis=0))
            at = (r + D) * 2 * LANES
            lhs[pl.ds(q, 16), at:at + LANES] = hi
            lhs[pl.ds(q, 16), at + LANES:at + 2 * LANES] = lo

    def body(g, x):
        p = pl.multiple_of(g * 16, 16)
        pair(p, p, True)
        return x

    lax.fori_loop(0, d.groups // 2, body, 0)
    pair(d.groups // 2 * 16, d.groups // 2 * 16, False)


def reduce_members(d, lhs, bsel, yo, yr):
    k0, k1, k2 = D * 2 * LANES, (D + d.r) * 2 * LANES, d.rr * 2 * LANES
    scale = KAPPA ** (2 * SWEEPS)
    dot = lambda a, b: jnp.dot(lhs[:, a:b], bsel[a:b, :], preferred_element_type=f32)
    yo[...] = dot(k0, k1) * scale
    yr[...] = (dot(0, k0) + dot(k1, k2)) * scale


def all_sum(x_ref, land, ssem, rsem):
    copies = []
    for k, (dy, dx) in enumerate(others()):
        copies.append(pltpu.make_async_remote_copy(
            src_ref=x_ref, dst_ref=land.at[k], send_sem=ssem.at[k], recv_sem=rsem.at[k],
            device_id=peer(dy, dx), device_id_type=MESH))
        copies[-1].start()
    for c in copies:
        c.wait_recv()
    total = x_ref[...]
    for k in range(len(copies)):
        total = total + land[k]
    return copies, total


def ens_send_rows(d, et, hn, hs):
    lane = lane_iota(d.cols)
    low = lane < LANES // 2
    at = lambda r: et[BASE + (r + D) * d.st + D:BASE + (r + D) * d.st + D + d.cols, :]
    for i in range(2):
        hn[i] = jnp.where(low, at(i), flip(at(i + 2)))
        hs[i] = jnp.where(low, flip(at(d.r - 2 + i)), at(d.r - 4 + i))


def main_kernel(d, ens_in, cell_in, level_in, inn_in, wt_in, p0_out, p1_out, ym_out, *refs):
    refs = list(refs)
    take = lambda n: [refs.pop(0) for _ in range(n)]
    ec, et, u, a1, a2, a3, pad, b1, b2, b3 = take(10)
    sel, bsel, lhs, po0, po1 = take(5)
    cm, rt, rb = masks = take(3)
    hn, hs, hw, he, ln, ls, lw, le, lnw, lne, lsw, lse, esem, rsem = take(14)
    go, gr, do, dr, g1o, g1r, y0o, y0r, y1o, y1r = take(10)
    ex0, ex1, ex2 = take(18), take(18), take(18)
    x_ref, sum_land, sum_s, sum_r = take(4)
    ens, cell, level, inn, wt, isem, osem = take(7)
    es = d.rows + 1
    gy, gx = lax.axis_index("gy"), lax.axis_index("gx")
    ny, nx = lax.axis_size("gy"), lax.axis_size("gx")
    flag = lambda b: jnp.where(b, 1.0, 0.0).astype(f32)
    hasn, hass, hasw, hase = flag(gy > 0), flag(gy < ny - 1), flag(gx > 0), flag(gx < nx - 1)

    meet_signal()
    chunk = d.members // 4
    loads = [pltpu.make_async_copy(ens_in.at[pl.ds(k * chunk, chunk)], ens.at[pl.ds(k * chunk, chunk)], isem.at[k])
             for k in range(4)]
    small = [pltpu.make_async_copy(a, b, isem.at[4 + k])
             for k, (a, b) in enumerate(((cell_in, cell), (level_in, level), (inn_in, inn), (wt_in, wt)))]
    for c in loads + small:
        c.start()
    for n, refs_n in enumerate(((ln,), (ls,), (lw,), (le,), (lnw,), (lne,), (lsw,), (lse,))):
        clear_absent(n, refs_n + tuple(ex[8 + n] for ex in (ex0, ex1, ex2)))

    def convert(k, x):
        for l in range(d.levels):
            ec[pl.ds((k * d.levels + l) * es, d.rows), :] = ens[k, l].astype(f32)
        return x

    for k in range(4):
        loads[k].wait()
        lax.fori_loop(k * chunk, (k + 1) * chunk, convert, 0)

    def transpose_row(r):
        parts = []
        for h in range(d.halves):
            for f in range(0, d.fields, 8):
                parts.append(ec[pl.ds(f * es + h * d.r + r, 8, stride=es), :])
        et[pl.ds(BASE + (r + D) * d.st + D, d.cols), :] = jnp.concatenate(parts, axis=0).T

    def transpose_four(q):
        for t in range(4):
            transpose_row(q * 4 + t)
        for t in range(4):
            r = q * 4 + t
            at = BASE + (r + D) * d.st + D
            to = pl.ds(pl.multiple_of(r * 4, 4), 4)
            hw[to, :] = et[pl.ds(at, 4), :]
            he[to, :] = et[pl.ds(at + d.cols - 4, 4), :]

    lax.fori_loop(0, d.r // 4, lambda q, x: (transpose_four(q), x)[1], 0)
    ens_send_rows(d, et, hn, hs)
    n4 = d.r * 4
    meet_wait()
    ecopies = [Side(N_, hn, ls, esem, rsem), Side(S_, hs, ln, esem, rsem),
               Side(W_, hw, le, esem, rsem), Side(E_, he, lw, esem, rsem),
               Side(NW, hw.at[0:16], lse, esem, rsem), Side(NE, he.at[0:16], lsw, esem, rsem),
               Side(SW, hw.at[n4 - 16:n4], lne, esem, rsem), Side(SE, he.at[n4 - 16:n4], lnw, esem, rsem)]
    for c in small:
        c.wait()

    scatter(d, cell, level, inn, wt, go, do)
    gr[...] = jnp.zeros_like(gr)
    dr[...] = jnp.zeros_like(dr)
    gcopies = exchange(d, [(go, gr), (do, dr)], ex0)
    build_selectors(d, sel, bsel)
    p = lax.broadcasted_iota(jnp.int32, (d.groups * 8, LANES), 0)
    cm[...] = jnp.where(p < D, hasw, jnp.where(p >= D + d.cols, hase, 1.0))
    low8 = lane_iota(8) < LANES // 2
    rt[...] = jnp.where(low8, hasn, 1.0)
    rb[...] = jnp.where(low8, 1.0, hass)

    zero = lambda n: jnp.zeros((n, LANES), f32)
    for ref, ext in ((pad, 0), (b1, 1), (b2, 2), (b3, 3)):
        for r in range(-min(ext + 2, D), d.r + min(ext + 2, D)):
            at = BASE + (r + D) * d.st
            if r < -ext or r >= d.r + ext:
                ref[at:at + d.st, :] = zero(d.st)
            else:
                ref[at + d.groups * 8:at + d.st, :] = zero(d.st - d.groups * 8)
                if ext == 0:
                    ref[at:at + D, :] = zero(D)
                    ref[at + D + d.cols:at + d.groups * 8, :] = zero(D)
        ref[0:BASE, :] = zero(BASE)
        ref[BASE + d.rr * d.st:d.size, :] = zero(8)

    for c in ecopies:
        c.wait_recv()
    low = lane_iota(d.cols) < LANES // 2
    row_at = lambda r: BASE + (r + D) * d.st
    own = lambda r: et[row_at(r) + D:row_at(r) + D + d.cols, :]
    for j in range(D):
        south = ls[j % 2]
        north = ln[j % 2]
        if j < 2:
            sv = flip(jnp.where(low, south, own(j)))
            nv = flip(jnp.where(low, own(d.r - 4 + j), north))
        else:
            sv = jnp.where(low, flip(own(j)), south)
            nv = jnp.where(low, north, flip(own(d.r - 4 + j)))
        et[row_at(d.r + j) + D:row_at(d.r + j) + D + d.cols, :] = sv
        et[row_at(j - D) + D:row_at(j - D) + D + d.cols, :] = nv
    low16 = lane_iota(16) < LANES // 2
    for land, north, south, off in ((lw, lnw, lsw, 0), (le, lne, lse, D + d.cols)):
        for r in range(d.r):
            et[row_at(r) + off:row_at(r) + off + 4, :] = land[r * 4:r * 4 + 4, :]
        nv = flip(jnp.where(low16, land[n4 - 16:n4, :], north[...]))
        sv = flip(jnp.where(low16, south[...], land[0:16, :]))
        for j in range(D):
            et[row_at(j - D) + off:row_at(j - D) + off + 4, :] = nv[j * 4:j * 4 + 4, :]
            et[row_at(d.r + j) + off:row_at(d.r + j) + off + 4, :] = sv[j * 4:j * 4 + 4, :]

    def g_step(g_o, g_r, po, out, n, yo, yr):
        expand(d, g_o, g_r, sel, et, u)
        half_filter(d, u, (a1, a2, a3), pad, po, masks)
        copy = pltpu.make_async_copy(po, out, osem.at[n])
        copy.start()
        back_filter(d, pad, (b1, b2, b3), et, lhs, masks)
        reduce_members(d, lhs, bsel, yo, yr)
        return copy

    o0 = g_step(go, gr, po0, p0_out, 0, y0o, y0r)
    ycopies = exchange(d, [(y0o, y0r)], ex1)
    g1o[...] = do[...] * y0o[...]
    g1r[...] = dr[...] * y0r[...]
    o1 = g_step(g1o, g1r, po1, p1_out, 1, y1o, y1r)
    zcopies = exchange(d, [(y1o, y1r)], ex2)
    inner = slice(D, D + d.cols)
    y0, y1, g0, g1, dd = y0o[inner, :], y1o[inner, :], go[inner, :], g1o[inner, :], do[inner, :]
    lane1 = lane_iota(1)
    x = jnp.zeros((1, LANES), f32)
    for k, v in enumerate((g0 * y0, g1 * y0, g1 * y1, dd * y1 * y1)):
        t = jnp.sum(jnp.sum(v, axis=0, keepdims=True), axis=1, keepdims=True)
        x = jnp.where(lane1 == k, t, x)
    x_ref[...] = x
    ym_out[0:d.cols, :] = y0
    ym_out[d.cols:2 * d.cols, :] = y1
    scopies, total = all_sum(x_ref, sum_land, sum_s, sum_r)
    ym_out[2 * d.cols:2 * d.cols + 8, :] = jnp.broadcast_to(total, (8, LANES))
    for c in ecopies + gcopies + ycopies + zcopies + scopies:
        c.wait_send()
    o0.wait()
    o1.wait()


def final_kernel(d, p0, p1, ym, c_ref, inc_ref):
    y0, y1, m = ym[0:d.cols], ym[d.cols:2 * d.cols], ym[2 * d.cols:2 * d.cols + 1]
    m = [m[:, k:k + 1] for k in range(4)]
    bn2 = m[0] + EPS
    c = (EPS - m[1]) / bn2
    alpha1 = (m[0] + m[1]) / bn2
    r2 = jnp.maximum((c * c * m[0] + 2.0 * c * m[1] + m[2]) / bn2, 0.0)
    rho = (c * c * m[1] + 2.0 * c * m[2] + m[3]) / bn2
    b2 = r2 + EPS
    alpha2 = (r2 + rho) / b2
    det = alpha1 * alpha2 - b2
    ca, cb = (alpha2 - c) / det, -1.0 / det
    wide = lambda v: jnp.broadcast_to(v, (LANES, LANES))
    scale = KAPPA ** SWEEPS
    sa, sb = wide(ca * scale), wide(cb * scale)
    inc = (wide(ca) * y0 + wide(cb) * y1).T
    for l in range(d.levels):
        inc_ref[l] = inc[l * d.rows:(l + 1) * d.rows]
    step = p0.shape[0]
    for r in range(step):
        v = (sa * p0[r] + sb * p1[r]).T
        for h in range(d.halves):
            for f in range(0, d.fields, 8):
                at = h * d.fields + f
                c_ref[pl.ds((f * d.halves + h) * step + r, 8, stride=d.halves * step), :] = v[at:at + 8]


def on_device(ensemble, obs_cell, obs_level, innovation, obs_weight):
    members, levels, rows, cols = ensemble.shape
    d = Dims(members, levels, rows, cols)
    nx, ny = lax.axis_size("gx"), lax.axis_size("gy")
    vm = pl.BlockSpec(memory_space=pltpu.VMEM)
    hbm = pl.BlockSpec(memory_space=pltpu.HBM)
    dma = pltpu.SemaphoreType.DMA
    v = lambda *s: pltpu.VMEM(s, f32)
    flat = lambda a: a.reshape(1, -1)
    shape = lambda *s: jax.ShapeDtypeStruct(s, f32)
    scratch = [v(d.fields * (rows + 1), LANES)] + [v(d.size, LANES)] * 9
    scratch += [pltpu.VMEM((d.rr // 2, 256, 256), bf16), pltpu.VMEM((d.rr * 256, LANES), bf16),
                pltpu.VMEM((d.st, d.rr * 256), bf16), v(d.r, cols, LANES), v(d.r, cols, LANES)]
    scratch += [v(d.groups * 8, LANES), v(8, LANES), v(8, LANES)]
    side = d.r * 4
    scratch += [v(2, cols, LANES), v(2, cols, LANES), v(side, LANES), v(side, LANES)] * 2
    scratch += [v(16, LANES)] * 4 + [dma((8,)), dma((8,))]
    scratch += [v(d.st, LANES)] * 10
    scratch += exchange_buffers(2) + exchange_buffers(1) + exchange_buffers(1)
    n = nx * ny - 1
    obs = obs_cell.shape[-1]
    scratch += [v(1, LANES), v(n, 1, LANES), dma((n,)), dma((n,))]
    scratch += [pltpu.VMEM(ensemble.shape, bf16)] + [pltpu.VMEM((1, obs), jnp.int32)] * 2 + [v(1, obs)] * 2
    scratch += [dma((8,)), dma((2,))]

    def main_entry(*refs):
        main_kernel(d, *refs)

    p0, p1, ym = pl.pallas_call(
        main_entry,
        out_shape=(shape(d.r, cols, LANES), shape(d.r, cols, LANES), shape(2 * cols + 8, LANES)),
        in_specs=[hbm] * 5,
        out_specs=(hbm, hbm, vm),
        scratch_shapes=scratch,
        compiler_params=pltpu.CompilerParams(collective_id=0, has_side_effects=True, vmem_limit_bytes=64000000),
    )(ensemble, flat(obs_cell), flat(obs_level), flat(innovation), flat(obs_weight))
    step = 8
    block = d.fields * d.halves * step
    full = lambda *s: pl.BlockSpec(s, lambda i: (0,) * len(s))
    out4 = (d.r // step, block, LANES)

    def final_grid(p0, p1, ym, c_ref, inc_ref, buf, sem):
        i = pl.program_id(0)
        steps = pl.num_programs(0)
        slot = lax.rem(i, 2)

        def copy(j, k):
            return pltpu.make_async_copy(
                buf.at[k].reshape(d.fields * d.halves, step, LANES),
                c_ref.at[:, pl.ds(pl.multiple_of(j * step, step), step), :], sem.at[k])

        @pl.when(i >= 2)
        def _():
            copy(i - 2, slot).wait()

        final_kernel(d, p0, p1, ym, buf.at[slot], inc_ref)
        copy(i, slot).start()

        @pl.when(i == steps - 1)
        def _():
            copy(i - 1, 1 - slot).wait()
            copy(i, slot).wait()

    control, increment = pl.pallas_call(
        final_grid,
        grid=(d.r // step,),
        out_shape=(shape(d.fields * d.halves, d.r, LANES), shape(levels, rows, cols)),
        in_specs=[pl.BlockSpec((step, cols, LANES), lambda i: (i, 0, 0))] * 2 + [full(2 * cols + 8, LANES)],
        out_specs=(hbm, full(levels, rows, cols)),
        scratch_shapes=[v(2, block, LANES), dma((2,))],
        compiler_params=pltpu.CompilerParams(vmem_limit_bytes=64000000),
    )(p0, p1, ym)
    return (control.reshape(members, levels, rows, cols), increment)


def solution(mesh):
    return jax.shard_map(
        on_device,
        mesh=mesh,
        in_specs=(
            P(None, None, "gy", "gx"),
            P("gy", "gx", None),
            P("gy", "gx", None),
            P("gy", "gx", None),
            P("gy", "gx", None),
        ),
        out_specs=(P(None, None, "gy", "gx"), P(None, "gy", "gx")),
        check_vma=False,
    )
```

```python
import math
import jax
import jax.numpy as jnp
from jax import lax
from jax.experimental import pallas as pl
from jax.experimental.pallas import tpu as pltpu
from jax.sharding import PartitionSpec as P

SWEEPS = 4
KAPPA = 0.2
EPS = 1e-06
D = SWEEPS
BASE = 8
LANES = 128
SIDES = [(-1, 0), (1, 0), (0, -1), (0, 1), (-1, -1), (-1, 1), (1, -1), (1, 1)]
N_, S_, W_, E_, NW, NE, SW, SE = range(8)
BACK = [S_, N_, E_, W_, SE, SW, NE, NW]
MESH = pl.DeviceIdType.MESH
f32, bf16 = jnp.float32, jnp.bfloat16


class Dims:
    def __init__(self, members, levels, rows, cols):
        self.members, self.levels, self.rows, self.cols = members, levels, rows, cols
        self.fields = members * levels
        self.halves = LANES // self.fields
        assert self.halves == 2 and cols == LANES and levels * rows == LANES
        self.r = rows // self.halves
        self.rr = self.r + 2 * D
        self.groups = (cols + 2 * D) // 8
        self.st = -(-(cols + 2 * D) // 16) * 16
        self.size = BASE + self.rr * self.st + 8


def peer(dy, dx):
    ny, nx = lax.axis_size("gy"), lax.axis_size("gx")
    return {"gy": lax.rem(lax.axis_index("gy") + dy + ny, ny), "gx": lax.rem(lax.axis_index("gx") + dx + nx, nx)}


def others():
    ny, nx = lax.axis_size("gy"), lax.axis_size("gx")
    return [(dy, dx) for dy in range(ny) for dx in range(nx) if dy or dx]


def meet_signal():
    bar = pltpu.get_barrier_semaphore()
    for dy, dx in others():
        pl.semaphore_signal(bar, inc=1, device_id=peer(dy, dx), device_id_type=MESH)


def meet_wait():
    pl.semaphore_wait(pltpu.get_barrier_semaphore(), len(others()))


def present(n):
    dy, dx = SIDES[n]
    gy, gx = lax.axis_index("gy") + dy, lax.axis_index("gx") + dx
    ok = None
    for d, i, axis in ((dy, gy, "gy"), (dx, gx, "gx")):
        if d:
            t = (i >= 0) if d < 0 else (i < lax.axis_size(axis))
            ok = t if ok is None else ok & t
    return ok


class Side:
    def __init__(self, n, src, dst, ssem, rsem):
        dy, dx = SIDES[n]
        self.n = n
        self.copy = pltpu.make_async_remote_copy(src_ref=src, dst_ref=dst, send_sem=ssem.at[n], recv_sem=rsem.at[n],
                                                 device_id=peer(dy, dx), device_id_type=MESH)
        pl.when(present(n))(self.copy.start)

    def wait_recv(self):
        pl.when(present(BACK[self.n]))(self.copy.wait_recv)

    def wait_send(self):
        pl.when(present(self.n))(self.copy.wait_send)


def clear_absent(n, refs):
    @pl.when(jnp.logical_not(present(n)))
    def _():
        for ref in refs:
            ref[...] = jnp.zeros_like(ref)


def lane_iota(rows):
    return lax.broadcasted_iota(jnp.int32, (rows, LANES), 1)


def flip(x):
    return pltpu.roll(x, LANES // 2, 1)


def scatter(d, cell_ref, level_ref, inn_ref, wt_ref, go, do):
    cell = cell_ref[...]
    row = level_ref[...] * d.rows + cell // d.cols
    col = cell % d.cols
    n = cell.shape[1]
    hot = jnp.where(lax.broadcasted_iota(jnp.int32, (d.levels * d.rows, n), 0) == row, 1.0, 0.0).astype(bf16)
    at = lax.broadcasted_iota(jnp.int32, (d.cols, n), 0) == col
    wt = wt_ref[...]
    for ref, v in ((go, wt * inn_ref[...]), (do, wt)):
        hi = v.astype(bf16).astype(f32)
        total = None
        for part in (hi, v - hi):
            sel = jnp.where(at, part, 0.0).astype(bf16)
            term = lax.dot_general(sel, hot, (((1,), (1,)), ((), ())), preferred_element_type=f32)
            total = term if total is None else total + term
        ref[D:D + d.cols, :] = total
        ref[0:D, :] = jnp.zeros((D, LANES), f32)
        ref[D + d.cols:d.st, :] = jnp.zeros((d.st - D - d.cols, LANES), f32)


def row_masks(d, rows):
    rowl = lane_iota(rows) % d.rows
    return rowl < D, rowl >= d.rows - D, (rowl >= d.r - D) & (rowl < d.r + D)


def exchange_buffers(n):
    v = lambda *s: pltpu.VMEM((n,) + s, f32)
    one = [v(3, 8, LANES)] * 2 + [v(2, 8, LANES)] * 2 + [v(8, LANES)] * 4
    dma = pltpu.SemaphoreType.DMA
    return one + one + [dma((8,)), dma((8,))]


def exchange_start(d, pairs, bufs):
    out, land, ssem, rsem = bufs[:8], bufs[8:16], bufs[16], bufs[17]
    lo, hi, mid = row_masks(d, 8)
    last = d.groups - 1
    at = lambda g: slice(g * 8, g * 8 + 8)
    for a, (yo, yr) in enumerate(pairs):
        packs = [[None] * 3, [None] * 3]
        for g in range(d.groups):
            own, ring = yo[at(g), :], yr[at(g), :]
            own = own + jnp.where(mid, ring, 0.0)
            yo[at(g), :] = own
            for k in range(2):
                v = jnp.where(lo, own if k == 0 else ring, jnp.where(hi, ring if k == 0 else own, 0.0))
                if g == 0:
                    out[NW + 2 * k][a] = v
                if g == last:
                    out[NE + 2 * k][a] = v
                v = pltpu.roll(v, D + 8 * (g % 8), 1)
                packs[k][g // 8] = v if packs[k][g // 8] is None else packs[k][g // 8] + v
            if g == 0 or g == last:
                m = out[W_ if g == 0 else E_]
                m[a, 0] = own
                m[a, 1] = ring
        for k in range(2):
            for j in range(3):
                out[k][a, j] = packs[k][j]
    return [Side(n, out[n], land[BACK[n]], ssem, rsem) for n in (N_, S_, W_, E_, NW, NE, SW, SE)]


def exchange_finish(d, pairs, bufs, copies):
    land = bufs[8:16]
    lo, hi, mid = row_masks(d, 8)
    last = d.groups - 1
    at = lambda g: slice(g * 8, g * 8 + 8)
    for c in copies:
        c.wait_recv()
    for a, (yo, yr) in enumerate(pairs):
        for g in range(d.groups):
            own, ring = yo[at(g), :], yr[at(g), :]
            shift = (LANES - D - 8 * (g % 8)) % LANES
            north = pltpu.roll(land[N_][a, g // 8], shift, 1)
            south = pltpu.roll(land[S_][a, g // 8], shift, 1)
            if g == 0:
                north, south = north + land[NW][a], south + land[SW][a]
            if g == last:
                north, south = north + land[NE][a], south + land[SE][a]
            if g == 0 or g == last:
                m = land[W_ if g == 0 else E_]
                own, ring = own + m[a, 0], ring + m[a, 1]
            own = own + jnp.where(lo, north, jnp.where(hi, south, 0.0))
            ring = ring + jnp.where(hi, north, jnp.where(lo, south, 0.0))
            yo[at(g), :] = own
            yr[at(g), :] = jnp.where(mid, own, ring)


def build_selectors(d, sel, bsel):
    def code(x_iota, l_iota):
        level = x_iota // d.rows
        half = l_iota // d.fields
        base = lax.rem(lax.rem(x_iota, d.rows) - d.r * half + d.rows, d.rows)
        return jnp.where(lax.rem(l_iota, d.levels) == level, base, -1)

    a = lax.broadcasted_iota(jnp.int32, (LANES, LANES), 0)
    b = lax.broadcasted_iota(jnp.int32, (LANES, LANES), 1)
    for_sel, for_bsel = code(a, b), code(b, a)

    def fill(q, x):
        for s in range(2):
            i = q * 2 + s
            want = lax.rem(i - D + d.rows, d.rows)
            one = jnp.where(for_sel == want, 1.0, 0.0).astype(bf16)
            two = jnp.where(for_bsel == want, 1.0, 0.0).astype(bf16)
            for k in range(2):
                sel[q, k * LANES:(k + 1) * LANES, s * LANES:(s + 1) * LANES] = one
                bsel[pl.ds(pl.multiple_of(i * 256 + k * LANES, LANES), LANES), :] = two
        return x

    lax.fori_loop(0, d.rr // 2, fill, 0)


def split(x):
    hi = x.astype(bf16)
    return hi, (x - hi.astype(f32)).astype(bf16)


def wide(ref):
    hi, lo = split(ref[...])
    return jnp.concatenate([hi, lo], axis=1)


def expand(d, x, pairs, sel, et, u):
    n = d.groups * 8
    for q in pairs:
        g2 = jnp.dot(x, sel[q], preferred_element_type=f32)
        for s in range(2):
            at = BASE + (2 * q + s) * d.st
            u[at:at + n, :] = et[at:at + n, :] * g2[0:n, s * LANES:(s + 1) * LANES]


def expand_edges(d, x, pairs, sel, et, u):
    n = d.groups * 8
    x = jnp.concatenate([x[0:8], x[n - 8:n]], axis=0)
    for q in pairs:
        g2 = jnp.dot(x, sel[q], preferred_element_type=f32)
        for s in range(2):
            for k in range(2):
                at = BASE + (2 * q + s) * d.st + k * (n - 8)
                u[at:at + 8, :] = et[at:at + 8, :] * g2[k * 8:k * 8 + 8, s * LANES:(s + 1) * LANES]


def stencil(d, src, p, lo, hi, use):
    def ld(r, o):
        return src[pl.ds(p + (BASE + (r + D) * d.st + o), 8), :]

    n, c = ld(lo - 1, 0), ld(lo, 0)
    for r in range(lo, hi):
        s = ld(r + 1, 0)
        use(r, (n + s) + (c + (ld(r, -1) + ld(r, 1))))
        n, c = c, s


def sweep(d, src, dst, ext, masks):
    cm, rt, rb = masks

    def body(g, x):
        p = pl.multiple_of(g * 8, 8)
        m = cm[pl.ds(p, 8), :]
        mt, mb = m * rt[...], m * rb[...]

        def use(r, v):
            dst[pl.ds(p + (BASE + (r + D) * d.st), 8), :] = v * (mt if r < 0 else mb if r >= d.r else m)

        stencil(d, src, p, -ext, d.r + ext, use)
        return x

    lax.fori_loop(0, d.groups, body, 0)


def sweep_part(d, src, dst, ranges, groups, masks):
    def body(g, x):
        p = pl.multiple_of(groups[0] * 8 + g * (groups[1] * 8), 8)
        if masks is not None:
            cm, rt, rb = masks
            m = cm[pl.ds(p, 8), :]
            mt, mb = m * rt[...], m * rb[...]

        def use(r, v):
            if masks is not None:
                v = v * (mt if r < 0 else mb if r >= d.r else m)
            dst[pl.ds(p + (BASE + (r + D) * d.st), 8), :] = v

        for lo, hi in ranges:
            stencil(d, src, p, lo, hi, use)
        return x

    lax.fori_loop(0, groups[2], body, 0)


def last_part(d, src, pad, po, ranges, groups):
    def body(g, x):
        c = pl.multiple_of(groups[0] * 8 + g * (groups[1] * 8), 8)

        def use(r, v):
            pad[pl.ds(c + (D + BASE + (r + D) * d.st), 8), :] = v
            po[r, pl.ds(c, 8), :] = v

        for lo, hi in ranges:
            stencil(d, src, c + D, lo, hi, use)
        return x

    lax.fori_loop(0, groups[2], body, 0)


def filter_inner(d, src, bufs, pad, po, margin):
    groups = (0, 1, d.groups) if margin == 0 else (1, 1, d.groups - 2)
    for k, dst in enumerate(bufs):
        m = margin + k + 1
        sweep_part(d, src, dst, [(m, d.r - m)], groups, None)
        src = dst
    m = margin + SWEEPS
    last_part(d, src, pad, po, [(m, d.r - m)], (1, 1, d.cols // 8 - 2))


def filter_outer(d, src, bufs, pad, po, margin, masks):
    for k, dst in enumerate(bufs):
        m, e = margin + k + 1, SWEEPS - k - 1
        w = 2 if margin else 1
        sweep_part(d, src, dst, [(-e, m), (d.r - m, d.r + e)], (w, 1, d.groups - 2 * w), masks)
        for t in range(w):
            sweep_part(d, src, dst, [(-e, d.r + e)], (t, d.groups - w, 2), masks)
        src = dst
    m = margin + SWEEPS
    n = d.cols // 8
    last_part(d, src, pad, po, [(0, m), (d.r - m, d.r)], (1, 1, n - 2))
    last_part(d, src, pad, po, [(0, d.r)], (0, n - 1, 2))


def back_filter(d, pad, bufs, et, lhs, masks):
    b1, b2, b3 = bufs
    sweep(d, pad, b1, 1, masks)
    sweep(d, b1, b2, 2, masks)
    sweep(d, b2, b3, 3, masks)
    zero = jnp.zeros((8, LANES), f32)

    def pair(p, q, both):
        def ld(r, o):
            return b3[pl.ds(p + (BASE + (r + D) * d.st + o), 8), :]

        n = [None, None]
        c = [ld(-D, 0), ld(-D, 8) if both else None]
        for r in range(-D, d.r + D):
            ts = []
            for k in range(2 if both else 1):
                o = 8 * k
                v = c[k] + (ld(r, o - 1) + ld(r, o + 1))
                s = None
                if r < d.r + D - 1:
                    s = ld(r + 1, o)
                    v = v + s
                if r > -D:
                    v = v + n[k]
                n[k], c[k] = c[k], s
                ts.append(v * et[pl.ds(p + (BASE + (r + D) * d.st + o), 8), :])
            if not both:
                ts.append(zero)
            hi, lo = split(jnp.concatenate(ts, axis=0))
            at = (r + D) * 2 * LANES
            lhs[pl.ds(q, 16), at:at + LANES] = hi
            lhs[pl.ds(q, 16), at + LANES:at + 2 * LANES] = lo

    def body(g, x):
        p = pl.multiple_of(g * 16, 16)
        pair(p, p, True)
        return x

    lax.fori_loop(0, d.groups // 2, body, 0)
    pair(d.groups // 2 * 16, d.groups // 2 * 16, False)


def reduce_members(d, lhs, bsel, yo, yr):
    k0, k1, k2 = D * 2 * LANES, (D + d.r) * 2 * LANES, d.rr * 2 * LANES
    scale = KAPPA ** (2 * SWEEPS)
    dot = lambda a, b: jnp.dot(lhs[:, a:b], bsel[a:b, :], preferred_element_type=f32)
    yo[...] = dot(k0, k1) * scale
    yr[...] = (dot(0, k0) + dot(k1, k2)) * scale


def all_sum(x_ref, land, ssem, rsem):
    copies = []
    for k, (dy, dx) in enumerate(others()):
        copies.append(pltpu.make_async_remote_copy(
            src_ref=x_ref, dst_ref=land.at[k], send_sem=ssem.at[k], recv_sem=rsem.at[k],
            device_id=peer(dy, dx), device_id_type=MESH))
        copies[-1].start()
    for c in copies:
        c.wait_recv()
    total = x_ref[...]
    for k in range(len(copies)):
        total = total + land[k]
    return copies, total


def ens_send_rows(d, et, hn, hs):
    lane = lane_iota(d.cols)
    low = lane < LANES // 2
    at = lambda r: et[BASE + (r + D) * d.st + D:BASE + (r + D) * d.st + D + d.cols, :]
    for i in range(2):
        hn[i] = jnp.where(low, at(i), flip(at(i + 2)))
        hs[i] = jnp.where(low, flip(at(d.r - 2 + i)), at(d.r - 4 + i))


def main_kernel(d, ens_in, cell_in, level_in, inn_in, wt_in, p0_out, p1_out, ym_out, *refs):
    refs = list(refs)
    take = lambda n: [refs.pop(0) for _ in range(n)]
    ec, et, u, a1, a2, a3, pad, b1, b2, b3 = take(10)
    sel, bsel, lhs = take(3)
    cm, rt, rb = masks = take(3)
    hn, hs, hw, he, ln, ls, lw, le, lnw, lne, lsw, lse, esem, rsem = take(14)
    go, gr, do, dr, g1o, g1r, y0o, y0r, y1o, y1r = take(10)
    ex0, ex1, ex2 = take(18), take(18), take(18)
    x_ref, sum_land, sum_s, sum_r = take(4)
    ens, cell, level, inn, wt, isem = take(6)
    es = d.rows + 1
    gy, gx = lax.axis_index("gy"), lax.axis_index("gx")
    ny, nx = lax.axis_size("gy"), lax.axis_size("gx")
    flag = lambda b: jnp.where(b, 1.0, 0.0).astype(f32)
    hasn, hass, hasw, hase = flag(gy > 0), flag(gy < ny - 1), flag(gx > 0), flag(gx < nx - 1)

    meet_signal()
    chunk = d.members // 4
    loads = [pltpu.make_async_copy(ens_in.at[pl.ds(k * chunk, chunk)], ens.at[pl.ds(k * chunk, chunk)], isem.at[k])
             for k in range(4)]
    small = [pltpu.make_async_copy(a, b, isem.at[4 + k])
             for k, (a, b) in enumerate(((cell_in, cell), (level_in, level), (inn_in, inn), (wt_in, wt)))]
    for c in loads + small:
        c.start()
    for n, refs_n in enumerate(((ln,), (ls,), (lw,), (le,), (lnw,), (lne,), (lsw,), (lse,))):
        clear_absent(n, refs_n + tuple(ex[8 + n] for ex in (ex0, ex1, ex2)))

    def convert(k, x):
        for l in range(d.levels):
            ec[pl.ds((k * d.levels + l) * es, d.rows), :] = ens[k, l].astype(f32)
        return x

    for k in range(4):
        loads[k].wait()
        lax.fori_loop(k * chunk, (k + 1) * chunk, convert, 0)

    def transpose_row(r):
        parts = []
        for h in range(d.halves):
            for f in range(0, d.fields, 8):
                parts.append(ec[pl.ds(f * es + h * d.r + r, 8, stride=es), :])
        et[pl.ds(BASE + (r + D) * d.st + D, d.cols), :] = jnp.concatenate(parts, axis=0).T

    def transpose_four(q):
        for t in range(4):
            transpose_row(q * 4 + t)
        for t in range(4):
            r = q * 4 + t
            at = BASE + (r + D) * d.st + D
            to = pl.ds(pl.multiple_of(r * 4, 4), 4)
            hw[to, :] = et[pl.ds(at, 4), :]
            he[to, :] = et[pl.ds(at + d.cols - 4, 4), :]

    lax.fori_loop(0, d.r // 4, lambda q, x: (transpose_four(q), x)[1], 0)
    ens_send_rows(d, et, hn, hs)
    n4 = d.r * 4
    meet_wait()
    ecopies = [Side(N_, hn, ls, esem, rsem), Side(S_, hs, ln, esem, rsem),
               Side(W_, hw, le, esem, rsem), Side(E_, he, lw, esem, rsem),
               Side(NW, hw.at[0:16], lse, esem, rsem), Side(NE, he.at[0:16], lsw, esem, rsem),
               Side(SW, hw.at[n4 - 16:n4], lne, esem, rsem), Side(SE, he.at[n4 - 16:n4], lnw, esem, rsem)]
    for c in small:
        c.wait()

    scatter(d, cell, level, inn, wt, go, do)
    gr[...] = jnp.zeros_like(gr)
    dr[...] = jnp.zeros_like(dr)
    gpairs = [(go, gr), (do, dr)]
    gcopies = exchange_start(d, gpairs, ex0)
    build_selectors(d, sel, bsel)
    edge = D // 2
    pairs = d.rr // 2
    ring_pairs = lambda n: list(range(n)) + list(range(pairs - n, pairs))
    a_bufs = (a1, a2, a3)
    expand(d, wide(go), range(edge, pairs - edge), sel, et, u)
    filter_inner(d, u, a_bufs, pad, p0_out, 0)
    p = lax.broadcasted_iota(jnp.int32, (d.groups * 8, LANES), 0)
    cm[...] = jnp.where(p < D, hasw, jnp.where(p >= D + d.cols, hase, 1.0))
    low8 = lane_iota(8) < LANES // 2
    rt[...] = jnp.where(low8, hasn, 1.0)
    rb[...] = jnp.where(low8, 1.0, hass)

    zero = lambda n: jnp.zeros((n, LANES), f32)
    for ref, ext in ((pad, 0), (b1, 1), (b2, 2), (b3, 3)):
        for r in range(-min(ext + 2, D), d.r + min(ext + 2, D)):
            at = BASE + (r + D) * d.st
            if r < -ext or r >= d.r + ext:
                ref[at:at + d.st, :] = zero(d.st)
            else:
                ref[at + d.groups * 8:at + d.st, :] = zero(d.st - d.groups * 8)
                if ext == 0:
                    ref[at:at + D, :] = zero(D)
                    ref[at + D + d.cols:at + d.groups * 8, :] = zero(D)
        ref[0:BASE, :] = zero(BASE)
        ref[BASE + d.rr * d.st:d.size, :] = zero(8)

    exchange_finish(d, gpairs, ex0, gcopies)
    for c in ecopies:
        c.wait_recv()
    low = lane_iota(d.cols) < LANES // 2
    row_at = lambda r: BASE + (r + D) * d.st
    own = lambda r: et[row_at(r) + D:row_at(r) + D + d.cols, :]
    for j in range(D):
        south = ls[j % 2]
        north = ln[j % 2]
        if j < 2:
            sv = flip(jnp.where(low, south, own(j)))
            nv = flip(jnp.where(low, own(d.r - 4 + j), north))
        else:
            sv = jnp.where(low, flip(own(j)), south)
            nv = jnp.where(low, north, flip(own(d.r - 4 + j)))
        et[row_at(d.r + j) + D:row_at(d.r + j) + D + d.cols, :] = sv
        et[row_at(j - D) + D:row_at(j - D) + D + d.cols, :] = nv
    low16 = lane_iota(16) < LANES // 2
    for land, north, south, off in ((lw, lnw, lsw, 0), (le, lne, lse, D + d.cols)):
        for r in range(d.r):
            et[row_at(r) + off:row_at(r) + off + 4, :] = land[r * 4:r * 4 + 4, :]
        nv = flip(jnp.where(low16, land[n4 - 16:n4, :], north[...]))
        sv = flip(jnp.where(low16, south[...], land[0:16, :]))
        for j in range(D):
            et[row_at(j - D) + off:row_at(j - D) + off + 4, :] = nv[j * 4:j * 4 + 4, :]
            et[row_at(d.r + j) + off:row_at(d.r + j) + off + 4, :] = sv[j * 4:j * 4 + 4, :]

    def g_rest(g_o, g_r, po, yo, yr, margin):
        own, ring = wide(g_o), wide(g_r)
        expand(d, ring, ring_pairs(edge), sel, et, u)
        if margin:
            expand(d, own, list(range(edge, 2 * edge)) + list(range(pairs - 2 * edge, pairs - edge)), sel, et, u)
        first = edge + margin // 2
        expand_edges(d, own, range(first, pairs - first), sel, et, u)
        filter_outer(d, u, a_bufs, pad, po, margin, masks)
        back_filter(d, pad, (b1, b2, b3), et, lhs, masks)
        reduce_members(d, lhs, bsel, yo, yr)

    g_rest(go, gr, p0_out, y0o, y0r, 0)
    ycopies = exchange_start(d, [(y0o, y0r)], ex1)
    g1o[...] = do[...] * y0o[...]
    expand(d, wide(g1o), range(2 * edge, pairs - 2 * edge), sel, et, u)
    filter_inner(d, u, a_bufs, pad, p1_out, D)
    exchange_finish(d, [(y0o, y0r)], ex1, ycopies)
    g1o[...] = do[...] * y0o[...]
    g1r[...] = dr[...] * y0r[...]
    g_rest(g1o, g1r, p1_out, y1o, y1r, D)
    zcopies = exchange_start(d, [(y1o, y1r)], ex2)
    exchange_finish(d, [(y1o, y1r)], ex2, zcopies)
    inner = slice(D, D + d.cols)
    y0, y1, g0, g1, dd = y0o[inner, :], y1o[inner, :], go[inner, :], g1o[inner, :], do[inner, :]
    lane1 = lane_iota(1)
    x = jnp.zeros((1, LANES), f32)
    for k, v in enumerate((g0 * y0, g1 * y0, g1 * y1, dd * y1 * y1)):
        t = jnp.sum(jnp.sum(v, axis=0, keepdims=True), axis=1, keepdims=True)
        x = jnp.where(lane1 == k, t, x)
    x_ref[...] = x
    ym_out[0:d.cols, :] = y0
    ym_out[d.cols:2 * d.cols, :] = y1
    scopies, total = all_sum(x_ref, sum_land, sum_s, sum_r)
    ym_out[2 * d.cols:2 * d.cols + 8, :] = jnp.broadcast_to(total, (8, LANES))
    for c in ecopies + gcopies + ycopies + zcopies + scopies:
        c.wait_send()


def final_kernel(d, step, p0, p1, ym, c_ref, inc_ref, buf, sem):
    y0, y1, m = ym[0:d.cols], ym[d.cols:2 * d.cols], ym[2 * d.cols:2 * d.cols + 1]
    m = [m[:, k:k + 1] for k in range(4)]
    bn2 = m[0] + EPS
    c = (EPS - m[1]) / bn2
    alpha1 = (m[0] + m[1]) / bn2
    r2 = jnp.maximum((c * c * m[0] + 2.0 * c * m[1] + m[2]) / bn2, 0.0)
    rho = (c * c * m[1] + 2.0 * c * m[2] + m[3]) / bn2
    b2 = r2 + EPS
    alpha2 = (r2 + rho) / b2
    det = alpha1 * alpha2 - b2
    ca, cb = (alpha2 - c) / det, -1.0 / det
    full = lambda v: jnp.broadcast_to(v, (LANES, LANES))
    scale = KAPPA ** SWEEPS
    sa, sb = full(ca * scale), full(cb * scale)

    def copy(j):
        return pltpu.make_async_copy(
            buf.at[j].reshape(d.fields * d.halves, step, LANES),
            c_ref.at[:, pl.ds(pl.multiple_of(j * step, step), step), :], sem.at[j])

    def chunk(j, x):
        for t in range(step):
            r = j * step + t
            v = (sa * p0[r] + sb * p1[r]).T
            for h in range(d.halves):
                for f in range(0, d.fields, 8):
                    at = h * d.fields + f
                    buf[j, pl.ds((f * d.halves + h) * step + t, 8, stride=d.halves * step), :] = v[at:at + 8]
        copy(j).start()
        return x

    steps = d.r // step
    lax.fori_loop(0, steps, chunk, 0)
    inc = (full(ca) * y0 + full(cb) * y1).T
    for l in range(d.levels):
        inc_ref[l] = inc[l * d.rows:(l + 1) * d.rows]
    for j in range(steps):
        copy(j).wait()


def on_device(ensemble, obs_cell, obs_level, innovation, obs_weight):
    members, levels, rows, cols = ensemble.shape
    d = Dims(members, levels, rows, cols)
    nx, ny = lax.axis_size("gx"), lax.axis_size("gy")
    vm = pl.BlockSpec(memory_space=pltpu.VMEM)
    hbm = pl.BlockSpec(memory_space=pltpu.HBM)
    dma = pltpu.SemaphoreType.DMA
    v = lambda *s: pltpu.VMEM(s, f32)
    flat = lambda a: a.reshape(1, -1)
    shape = lambda *s: jax.ShapeDtypeStruct(s, f32)
    scratch = [v(d.fields * (rows + 1), LANES)] + [v(d.size, LANES)] * 9
    scratch += [pltpu.VMEM((d.rr // 2, 256, 256), bf16), pltpu.VMEM((d.rr * 256, LANES), bf16),
                pltpu.VMEM((d.st, d.rr * 256), bf16)]
    scratch += [v(d.groups * 8, LANES), v(8, LANES), v(8, LANES)]
    side = d.r * 4
    scratch += [v(2, cols, LANES), v(2, cols, LANES), v(side, LANES), v(side, LANES)] * 2
    scratch += [v(16, LANES)] * 4 + [dma((8,)), dma((8,))]
    scratch += [v(d.st, LANES)] * 10
    scratch += exchange_buffers(2) + exchange_buffers(1) + exchange_buffers(1)
    n = nx * ny - 1
    obs = obs_cell.shape[-1]
    scratch += [v(1, LANES), v(n, 1, LANES), dma((n,)), dma((n,))]
    scratch += [pltpu.VMEM(ensemble.shape, bf16)] + [pltpu.VMEM((1, obs), jnp.int32)] * 2 + [v(1, obs)] * 2
    scratch += [dma((8,))]

    def main_entry(*refs):
        main_kernel(d, *refs)

    p0, p1, ym = pl.pallas_call(
        main_entry,
        out_shape=(shape(d.r, cols, LANES), shape(d.r, cols, LANES), shape(2 * cols + 8, LANES)),
        in_specs=[hbm] * 5,
        out_specs=(vm, vm, vm),
        scratch_shapes=scratch,
        compiler_params=pltpu.CompilerParams(collective_id=0, has_side_effects=True, vmem_limit_bytes=48000000),
    )(*[pltpu.with_memory_space_constraint(a, pltpu.HBM) for a in (
        ensemble, flat(obs_cell), flat(obs_level), flat(innovation), flat(obs_weight))])
    step = 8
    block = d.fields * d.halves * step

    def final_entry(*refs):
        final_kernel(d, step, *refs)

    control, increment = pl.pallas_call(
        final_entry,
        out_shape=(shape(d.fields * d.halves, d.r, LANES), shape(levels, rows, cols)),
        in_specs=[vm] * 3,
        out_specs=(hbm, vm),
        scratch_shapes=[v(d.r // step, block, LANES), dma((d.r // step,))],
        compiler_params=pltpu.CompilerParams(vmem_limit_bytes=16000000),
    )(p0, p1, ym)
    return (control.reshape(members, levels, rows, cols), increment)


def solution(mesh):
    return jax.shard_map(
        on_device,
        mesh=mesh,
        in_specs=(
            P(None, None, "gy", "gx"),
            P("gy", "gx", None),
            P("gy", "gx", None),
            P("gy", "gx", None),
            P("gy", "gx", None),
        ),
        out_specs=(P(None, None, "gy", "gx"), P(None, "gy", "gx")),
        check_vma=False,
    )
```

```python
import math
import jax
import jax.numpy as jnp
from jax import lax
from jax.experimental import pallas as pl
from jax.experimental.pallas import tpu as pltpu
from jax.sharding import PartitionSpec as P

SWEEPS = 4
KAPPA = 0.2
EPS = 1e-06
D = SWEEPS
BASE = 8
LANES = 128
SIDES = [(-1, 0), (1, 0), (0, -1), (0, 1), (-1, -1), (-1, 1), (1, -1), (1, 1)]
N_, S_, W_, E_, NW, NE, SW, SE = range(8)
BACK = [S_, N_, E_, W_, SE, SW, NE, NW]
MESH = pl.DeviceIdType.MESH
f32, bf16 = jnp.float32, jnp.bfloat16


class Dims:
    def __init__(self, members, levels, rows, cols):
        self.members, self.levels, self.rows, self.cols = members, levels, rows, cols
        self.fields = members * levels
        self.halves = LANES // self.fields
        assert self.halves == 2 and cols == LANES and levels * rows == LANES
        self.r = rows // self.halves
        self.rr = self.r + 2 * D
        self.groups = (cols + 2 * D) // 8
        self.st = -(-(cols + 2 * D) // 16) * 16
        self.size = BASE + self.rr * self.st + 8


def peer(dy, dx):
    ny, nx = lax.axis_size("gy"), lax.axis_size("gx")
    return {"gy": lax.rem(lax.axis_index("gy") + dy + ny, ny), "gx": lax.rem(lax.axis_index("gx") + dx + nx, nx)}


def others():
    ny, nx = lax.axis_size("gy"), lax.axis_size("gx")
    return [(dy, dx) for dy in range(ny) for dx in range(nx) if dy or dx]


def meet_signal():
    bar = pltpu.get_barrier_semaphore()
    for dy, dx in others():
        pl.semaphore_signal(bar, inc=1, device_id=peer(dy, dx), device_id_type=MESH)


def meet_wait():
    pl.semaphore_wait(pltpu.get_barrier_semaphore(), len(others()))


def present(n):
    dy, dx = SIDES[n]
    gy, gx = lax.axis_index("gy") + dy, lax.axis_index("gx") + dx
    ok = None
    for d, i, axis in ((dy, gy, "gy"), (dx, gx, "gx")):
        if d:
            t = (i >= 0) if d < 0 else (i < lax.axis_size(axis))
            ok = t if ok is None else ok & t
    return ok


class Side:
    def __init__(self, n, src, dst, ssem, rsem):
        dy, dx = SIDES[n]
        self.n = n
        self.copy = pltpu.make_async_remote_copy(src_ref=src, dst_ref=dst, send_sem=ssem.at[n], recv_sem=rsem.at[n],
                                                 device_id=peer(dy, dx), device_id_type=MESH)
        pl.when(present(n))(self.copy.start)

    def wait_recv(self):
        pl.when(present(BACK[self.n]))(self.copy.wait_recv)

    def wait_send(self):
        pl.when(present(self.n))(self.copy.wait_send)


def clear_absent(n, refs):
    @pl.when(jnp.logical_not(present(n)))
    def _():
        for ref in refs:
            ref[...] = jnp.zeros_like(ref)


def lane_iota(rows):
    return lax.broadcasted_iota(jnp.int32, (rows, LANES), 1)


def flip(x):
    return pltpu.roll(x, LANES // 2, 1)


def scatter(d, cell_ref, level_ref, inn_ref, wt_ref, go, do):
    cell = cell_ref[...]
    row = level_ref[...] * d.rows + cell // d.cols
    col = cell % d.cols
    n = cell.shape[1]
    hot = jnp.where(lax.broadcasted_iota(jnp.int32, (d.levels * d.rows, n), 0) == row, 1.0, 0.0).astype(bf16)
    at = lax.broadcasted_iota(jnp.int32, (d.cols, n), 0) == col
    wt = wt_ref[...]
    for ref, v in ((go, wt * inn_ref[...]), (do, wt)):
        hi = v.astype(bf16).astype(f32)
        total = None
        for part in (hi, v - hi):
            sel = jnp.where(at, part, 0.0).astype(bf16)
            term = lax.dot_general(sel, hot, (((1,), (1,)), ((), ())), preferred_element_type=f32)
            total = term if total is None else total + term
        ref[D:D + d.cols, :] = total
        ref[0:D, :] = jnp.zeros((D, LANES), f32)
        ref[D + d.cols:d.st, :] = jnp.zeros((d.st - D - d.cols, LANES), f32)


def row_masks(d, rows):
    rowl = lane_iota(rows) % d.rows
    return rowl < D, rowl >= d.rows - D, (rowl >= d.r - D) & (rowl < d.r + D)


def exchange_buffers(n):
    v = lambda *s: pltpu.VMEM((n,) + s, f32)
    one = [v(3, 8, LANES)] * 2 + [v(2, 8, LANES)] * 2 + [v(8, LANES)] * 4
    dma = pltpu.SemaphoreType.DMA
    return one + one + [dma((8,)), dma((8,))]


def exchange_pack(d, pairs, bufs):
    out = bufs[:8]
    lo, hi, mid = row_masks(d, 8)
    last = d.groups - 1
    at = lambda g: slice(g * 8, g * 8 + 8)
    for a, (yo, yr) in enumerate(pairs):
        packs = [[None] * 3, [None] * 3]
        for g in range(d.groups):
            own, ring = yo[at(g), :], yr[at(g), :]
            own = own + jnp.where(mid, ring, 0.0)
            yo[at(g), :] = own
            for k in range(2):
                v = jnp.where(lo, own if k == 0 else ring, jnp.where(hi, ring if k == 0 else own, 0.0))
                if g == 0:
                    out[NW + 2 * k][a] = v
                if g == last:
                    out[NE + 2 * k][a] = v
                v = pltpu.roll(v, D + 8 * (g % 8), 1)
                packs[k][g // 8] = v if packs[k][g // 8] is None else packs[k][g // 8] + v
            if g == 0 or g == last:
                m = out[W_ if g == 0 else E_]
                m[a, 0] = own
                m[a, 1] = ring
        for k in range(2):
            for j in range(3):
                out[k][a, j] = packs[k][j]


def exchange_send(bufs):
    out, land, ssem, rsem = bufs[:8], bufs[8:16], bufs[16], bufs[17]
    return [Side(n, out[n], land[BACK[n]], ssem, rsem) for n in range(len(SIDES))]


def exchange_start(d, pairs, bufs):
    exchange_pack(d, pairs, bufs)
    return exchange_send(bufs)


def exchange_finish(d, pairs, bufs, copies):
    land = bufs[8:16]
    lo, hi, mid = row_masks(d, 8)
    last = d.groups - 1
    at = lambda g: slice(g * 8, g * 8 + 8)
    for c in copies:
        c.wait_recv()
    for a, (yo, yr) in enumerate(pairs):
        for g in range(d.groups):
            own, ring = yo[at(g), :], yr[at(g), :]
            shift = (LANES - D - 8 * (g % 8)) % LANES
            north = pltpu.roll(land[N_][a, g // 8], shift, 1)
            south = pltpu.roll(land[S_][a, g // 8], shift, 1)
            if g == 0:
                north, south = north + land[NW][a], south + land[SW][a]
            if g == last:
                north, south = north + land[NE][a], south + land[SE][a]
            if g == 0 or g == last:
                m = land[W_ if g == 0 else E_]
                own, ring = own + m[a, 0], ring + m[a, 1]
            own = own + jnp.where(lo, north, jnp.where(hi, south, 0.0))
            ring = ring + jnp.where(hi, north, jnp.where(lo, south, 0.0))
            yo[at(g), :] = own
            yr[at(g), :] = jnp.where(mid, own, ring)


def build_selectors(d, sel, bsel):
    def code(x_iota, l_iota, shift):
        level = x_iota // d.rows
        half = l_iota // d.fields
        base = lax.rem(lax.rem(x_iota, d.rows) - d.r * half - shift + d.rows, d.rows)
        return jnp.where(lax.rem(l_iota, d.levels) == level, base, -1)

    a = lax.broadcasted_iota(jnp.int32, (LANES, LANES), 0)
    b = lax.broadcasted_iota(jnp.int32, (LANES, LANES), 1)
    for_sel = code(a, b, 0)
    for_bsel = code(b, a, lax.rem(a, d.fields) // (d.fields // 2))

    def fill(q, x):
        want = lax.rem(q * 2 - D + d.rows, d.rows)
        two = jnp.where(for_bsel == want, 1.0, 0.0).astype(bf16)
        for k in range(2):
            bsel[pl.ds(pl.multiple_of(q * 256 + k * LANES, LANES), LANES), :] = two
        for s in range(2):
            one = jnp.where(for_sel == want + s, 1.0, 0.0).astype(bf16)
            for k in range(2):
                sel[q, k * LANES:(k + 1) * LANES, s * LANES:(s + 1) * LANES] = one
        return x

    lax.fori_loop(0, d.rr // 2, fill, 0)


def split(x):
    hi = x.astype(bf16)
    return hi, (x - hi.astype(f32)).astype(bf16)


def wide(ref):
    hi, lo = split(ref[...])
    return jnp.concatenate([hi, lo], axis=1)


def expand(d, x, pairs, sel, et, u):
    n = d.groups * 8
    for q in pairs:
        g2 = jnp.dot(x, sel[q], preferred_element_type=f32)
        for s in range(2):
            at = BASE + (2 * q + s) * d.st
            u[at:at + n, :] = et[at:at + n, :] * g2[0:n, s * LANES:(s + 1) * LANES]


def expand_edges(d, x, pairs, sel, et, u):
    n = d.groups * 8
    x = jnp.concatenate([x[0:8], x[n - 8:n]], axis=0)
    for q in pairs:
        g2 = jnp.dot(x, sel[q], preferred_element_type=f32)
        for s in range(2):
            for k in range(2):
                at = BASE + (2 * q + s) * d.st + k * (n - 8)
                u[at:at + 8, :] = et[at:at + 8, :] * g2[k * 8:k * 8 + 8, s * LANES:(s + 1) * LANES]


def stencil(d, src, p, lo, hi, use):
    def ld(r, o):
        return src[pl.ds(p + (BASE + (r + D) * d.st + o), 8), :]

    n, c = ld(lo - 1, 0), ld(lo, 0)
    for r in range(lo, hi):
        s = ld(r + 1, 0)
        use(r, (n + s) + (c + (ld(r, -1) + ld(r, 1))))
        n, c = c, s


def spread(n, rows, body):
    k = min(n, 5, max(1, 80 // rows))

    def step(i, x):
        for t in range(k):
            body(i * k + t)
        return x

    if n > k:
        lax.fori_loop(0, n // k, step, 0)
        for t in range(n // k * k, n):
            body(t)
    else:
        for t in range(n):
            body(t)


def aligned(x, n):
    return x if isinstance(x, int) else pl.multiple_of(x, n)


def count(ranges):
    return sum(hi - lo for lo, hi in ranges)


def sweep_part(d, src, dst, ranges, groups, masks):
    def body(g):
        p = aligned(groups[0] * 8 + g * (groups[1] * 8), 8)
        if masks is not None:
            cm, rt, rb = masks
            m = cm[pl.ds(p, 8), :]
            mt, mb = m * rt[...], m * rb[...]

        def use(r, v):
            if masks is not None:
                v = v * (mt if r < 0 else mb if r >= d.r else m)
            dst[pl.ds(p + (BASE + (r + D) * d.st), 8), :] = v

        for lo, hi in ranges:
            stencil(d, src, p, lo, hi, use)

    spread(groups[2], count(ranges), body)


def last_part(d, src, pad, po, ranges, groups):
    def body(g):
        c = aligned(groups[0] * 8 + g * (groups[1] * 8), 8)

        def use(r, v):
            pad[pl.ds(c + (D + BASE + (r + D) * d.st), 8), :] = v
            po[r, pl.ds(c, 8), :] = v

        for lo, hi in ranges:
            stencil(d, src, c + D, lo, hi, use)

    spread(groups[2], count(ranges), body)


def filter_inner(d, src, bufs, pad, po, margin):
    groups = (0, 1, d.groups) if margin == 0 else (1, 1, d.groups - 2)
    for k, dst in enumerate(bufs):
        m = margin + k + 1
        sweep_part(d, src, dst, [(m, d.r - m)], groups, None)
        src = dst
    m = margin + SWEEPS
    last_part(d, src, pad, po, [(m, d.r - m)], (1, 1, d.cols // 8 - 2))


def filter_outer(d, src, bufs, pad, po, margin, masks):
    for k, dst in enumerate(bufs):
        m, e = margin + k + 1, SWEEPS - k - 1
        w = 2 if margin else 1
        sweep_part(d, src, dst, [(-e, m), (d.r - m, d.r + e)], (w, 1, d.groups - 2 * w), masks)
        for t in range(w):
            sweep_part(d, src, dst, [(-e, d.r + e)], (t, d.groups - w, 2), masks)
        src = dst
    m = margin + SWEEPS
    n = d.cols // 8
    last_part(d, src, pad, po, [(0, m), (d.r - m, d.r)], (1, 1, n - 2))
    last_part(d, src, pad, po, [(0, d.r)], (0, n - 1, 2))


def back_filter(d, pad, bufs, et, lhs, masks):
    src = pad
    for k, dst in enumerate(bufs):
        sweep_part(d, src, dst, [(-k - 1, d.r + k + 1)], (0, 1, d.groups), masks)
        src = dst
    zero = jnp.zeros((8, LANES), f32)
    first = lane_iota(8) % d.fields < d.fields // 2
    quarter = d.fields // 2

    def pair(p, both):
        def ld(r, o):
            return src[pl.ds(p + (BASE + (r + D) * d.st + o), 8), :]

        n = [None, None]
        c = [ld(-D, 0), ld(-D, 8) if both else None]
        even = None
        for r in range(-D, d.r + D):
            ts = []
            for k in range(2 if both else 1):
                o = 8 * k
                v = c[k] + (ld(r, o - 1) + ld(r, o + 1))
                s = None
                if r < d.r + D - 1:
                    s = ld(r + 1, o)
                    v = v + s
                if r > -D:
                    v = v + n[k]
                n[k], c[k] = c[k], s
                ts.append(v * et[pl.ds(p + (BASE + (r + D) * d.st + o), 8), :])
            if (r + D) % 2 == 0:
                even = ts
                continue
            folded = [jnp.where(first, a, b) + jnp.where(first, pltpu.roll(a, LANES - quarter, 1), pltpu.roll(b, quarter, 1))
                      for a, b in zip(even, ts)]
            if not both:
                folded.append(zero)
            hi, lo = split(jnp.concatenate(folded, axis=0))
            at = (r + D) // 2 * 2 * LANES
            lhs[pl.ds(p, 16), at:at + LANES] = hi
            lhs[pl.ds(p, 16), at + LANES:at + 2 * LANES] = lo

    def body(g, x):
        pair(pl.multiple_of(g * 16, 16), True)
        return x

    lax.fori_loop(0, d.groups // 2, body, 0)
    pair(d.groups // 2 * 16, False)


def reduce_members(d, lhs, bsel, yo, yr):
    k0, k1, k2 = D * LANES, (D + d.r) * LANES, d.rr * LANES
    scale = KAPPA ** (2 * SWEEPS)
    dot = lambda a, b: jnp.dot(lhs[:, a:b], bsel[a:b, :], preferred_element_type=f32)
    yo[...] = dot(k0, k1) * scale
    yr[...] = (dot(0, k0) + dot(k1, k2)) * scale


def all_sum(x_ref, land, ssem, rsem, meanwhile):
    copies = []
    for k, (dy, dx) in enumerate(others()):
        copies.append(pltpu.make_async_remote_copy(
            src_ref=x_ref, dst_ref=land.at[k], send_sem=ssem.at[k], recv_sem=rsem.at[k],
            device_id=peer(dy, dx), device_id_type=MESH))
        copies[-1].start()
    meanwhile()
    for c in copies:
        c.wait_recv()
    total = x_ref[...]
    for k in range(len(copies)):
        total = total + land[k]
    return copies, total


def ens_send_rows(d, et, hn, hs):
    lane = lane_iota(d.cols)
    low = lane < LANES // 2
    at = lambda r: et[BASE + (r + D) * d.st + D:BASE + (r + D) * d.st + D + d.cols, :]
    for i in range(2):
        hn[i] = jnp.where(low, at(i), flip(at(i + 2)))
        hs[i] = jnp.where(low, flip(at(d.r - 2 + i)), at(d.r - 4 + i))


def main_kernel(d, ens_in, cell_in, level_in, inn_in, wt_in, p0_out, p1_out, ym_out, *refs):
    refs = list(refs)
    take = lambda n: [refs.pop(0) for _ in range(n)]
    ec, et, u, a1, a2, a3, pad, b1, b2, b3 = take(10)
    sel, bsel, lhs, po0, po1 = take(5)
    cm, rt, rb = masks = take(3)
    hn, hs, hw, he, ln, ls, lw, le, lnw, lne, lsw, lse, esem, rsem = take(14)
    go, gr, do, dr, g1o, g1r, y0o, y0r, y1o, y1r = take(10)
    ex0, ex1, ex2 = take(18), take(18), take(18)
    x_ref, sum_land, sum_s, sum_r = take(4)
    ens, cell, level, inn, wt, isem = take(6)
    es = d.rows + 1
    gy, gx = lax.axis_index("gy"), lax.axis_index("gx")
    ny, nx = lax.axis_size("gy"), lax.axis_size("gx")
    flag = lambda b: jnp.where(b, 1.0, 0.0).astype(f32)
    hasn, hass, hasw, hase = flag(gy > 0), flag(gy < ny - 1), flag(gx > 0), flag(gx < nx - 1)

    meet_signal()
    chunk = d.members // 4
    loads = [pltpu.make_async_copy(ens_in.at[pl.ds(k * chunk, chunk)], ens.at[pl.ds(k * chunk, chunk)], isem.at[k])
             for k in range(4)]
    small = [pltpu.make_async_copy(a, b, isem.at[4 + k])
             for k, (a, b) in enumerate(((cell_in, cell), (level_in, level), (inn_in, inn), (wt_in, wt)))]
    for c in small + loads:
        c.start()
    for n, refs_n in enumerate(((ln,), (ls,), (lw,), (le,), (lnw,), (lne,), (lsw,), (lse,))):
        clear_absent(n, refs_n + tuple(ex[8 + n] for ex in (ex0, ex1, ex2)))
    for c in small:
        c.wait()
    scatter(d, cell, level, inn, wt, go, do)
    gr[...] = jnp.zeros_like(gr)
    dr[...] = jnp.zeros_like(dr)
    gpairs = [(go, gr), (do, dr)]
    exchange_pack(d, gpairs, ex0)

    def convert(k, x):
        for l in range(d.levels):
            ec[pl.ds((k * d.levels + l) * es, d.rows), :] = ens[k, l].astype(f32)
        return x

    for k in range(4):
        loads[k].wait()
        lax.fori_loop(k * chunk, (k + 1) * chunk, convert, 0)

    def transpose_row(r):
        parts = []
        for h in range(d.halves):
            for f in range(0, d.fields, 8):
                parts.append(ec[pl.ds(f * es + h * d.r + r, 8, stride=es), :])
        et[pl.ds(BASE + (r + D) * d.st + D, d.cols), :] = jnp.concatenate(parts, axis=0).T

    def transpose_four(q):
        for t in range(4):
            transpose_row(q * 4 + t)
        for t in range(4):
            r = q * 4 + t
            at = BASE + (r + D) * d.st + D
            to = pl.ds(pl.multiple_of(r * 4, 4), 4)
            hw[to, :] = et[pl.ds(at, 4), :]
            he[to, :] = et[pl.ds(at + d.cols - 4, 4), :]

    def transpose_edges(k, x):
        transpose_four(k * (d.r // 4 - 1))
        return x

    def transpose_two(k, x):
        transpose_four(k * 2 + 1)
        transpose_four(k * 2 + 2)
        return x

    lax.fori_loop(0, 2, transpose_edges, 0)
    ens_send_rows(d, et, hn, hs)
    n4 = d.r * 4
    meet_wait()
    gcopies = exchange_send(ex0)
    ecopies = [Side(N_, hn, ls, esem, rsem), Side(S_, hs, ln, esem, rsem)]
    lax.fori_loop(0, d.r // 8 - 1, transpose_two, 0)
    ecopies += [Side(W_, hw, le, esem, rsem), Side(E_, he, lw, esem, rsem),
                Side(NW, hw.at[0:16], lse, esem, rsem), Side(NE, he.at[0:16], lsw, esem, rsem),
                Side(SW, hw.at[n4 - 16:n4], lne, esem, rsem), Side(SE, he.at[n4 - 16:n4], lnw, esem, rsem)]
    build_selectors(d, sel, bsel)
    edge = D // 2
    pairs = d.rr // 2
    ring_pairs = lambda n: list(range(n)) + list(range(pairs - n, pairs))
    a_bufs = (a1, a2, a3)
    expand(d, wide(go), range(edge, pairs - edge), sel, et, u)
    filter_inner(d, u, a_bufs, pad, po0, 0)
    p = lax.broadcasted_iota(jnp.int32, (d.groups * 8, LANES), 0)
    cm[...] = jnp.where(p < D, hasw, jnp.where(p >= D + d.cols, hase, 1.0))
    low8 = lane_iota(8) < LANES // 2
    rt[...] = jnp.where(low8, hasn, 1.0)
    rb[...] = jnp.where(low8, 1.0, hass)

    zero = lambda n: jnp.zeros((n, LANES), f32)
    for ref, ext in ((pad, 0), (b1, 1), (b2, 2), (b3, 3)):
        for r in range(-min(ext + 2, D), d.r + min(ext + 2, D)):
            at = BASE + (r + D) * d.st
            if r < -ext or r >= d.r + ext:
                ref[at:at + d.st, :] = zero(d.st)
            else:
                ref[at + d.groups * 8:at + d.st, :] = zero(d.st - d.groups * 8)
                if ext == 0:
                    ref[at:at + D, :] = zero(D)
                    ref[at + D + d.cols:at + d.groups * 8, :] = zero(D)
        ref[0:BASE, :] = zero(BASE)
        ref[BASE + d.rr * d.st:d.size, :] = zero(8)

    exchange_finish(d, gpairs, ex0, gcopies)
    for c in ecopies:
        c.wait_recv()
    low = lane_iota(d.cols) < LANES // 2
    row_at = lambda r: BASE + (r + D) * d.st
    own = lambda r: et[row_at(r) + D:row_at(r) + D + d.cols, :]
    for j in range(D):
        south = ls[j % 2]
        north = ln[j % 2]
        if j < 2:
            sv = flip(jnp.where(low, south, own(j)))
            nv = flip(jnp.where(low, own(d.r - 4 + j), north))
        else:
            sv = jnp.where(low, flip(own(j)), south)
            nv = jnp.where(low, north, flip(own(d.r - 4 + j)))
        et[row_at(d.r + j) + D:row_at(d.r + j) + D + d.cols, :] = sv
        et[row_at(j - D) + D:row_at(j - D) + D + d.cols, :] = nv
    low16 = lane_iota(16) < LANES // 2
    for land, north, south, off in ((lw, lnw, lsw, 0), (le, lne, lse, D + d.cols)):
        for r in range(d.r):
            et[row_at(r) + off:row_at(r) + off + 4, :] = land[r * 4:r * 4 + 4, :]
        nv = flip(jnp.where(low16, land[n4 - 16:n4, :], north[...]))
        sv = flip(jnp.where(low16, south[...], land[0:16, :]))
        for j in range(D):
            et[row_at(j - D) + off:row_at(j - D) + off + 4, :] = nv[j * 4:j * 4 + 4, :]
            et[row_at(d.r + j) + off:row_at(d.r + j) + off + 4, :] = sv[j * 4:j * 4 + 4, :]

    def g_rest(g_o, g_r, po, yo, yr, margin):
        own, ring = wide(g_o), wide(g_r)
        expand(d, ring, ring_pairs(edge), sel, et, u)
        if margin:
            expand(d, own, list(range(edge, 2 * edge)) + list(range(pairs - 2 * edge, pairs - edge)), sel, et, u)
        first = edge + margin // 2
        expand_edges(d, own, range(first, pairs - first), sel, et, u)
        filter_outer(d, u, a_bufs, pad, po, margin, masks)
        back_filter(d, pad, (b1, b2, b3), et, lhs, masks)
        reduce_members(d, lhs, bsel, yo, yr)

    g_rest(go, gr, po0, y0o, y0r, 0)
    ycopies = exchange_start(d, [(y0o, y0r)], ex1)
    g1o[...] = do[...] * y0o[...]
    expand(d, wide(g1o), range(2 * edge, pairs - 2 * edge), sel, et, u)
    filter_inner(d, u, a_bufs, pad, po1, D)
    exchange_finish(d, [(y0o, y0r)], ex1, ycopies)
    g1o[...] = do[...] * y0o[...]
    g1r[...] = dr[...] * y0r[...]
    g_rest(g1o, g1r, po1, y1o, y1r, D)
    zcopies = exchange_start(d, [(y1o, y1r)], ex2)
    exchange_finish(d, [(y1o, y1r)], ex2, zcopies)
    inner = slice(D, D + d.cols)
    y0, y1, g0, g1, dd = y0o[inner, :], y1o[inner, :], go[inner, :], g1o[inner, :], do[inner, :]
    lane1 = lane_iota(1)
    x = jnp.zeros((1, LANES), f32)
    for k, v in enumerate((g0 * y0, g1 * y0, g1 * y1, dd * y1 * y1)):
        t = jnp.sum(jnp.sum(v, axis=0, keepdims=True), axis=1, keepdims=True)
        x = jnp.where(lane1 == k, t, x)
    x_ref[...] = x

    def meanwhile():
        ym_out[0:d.cols, :] = y0.T
        ym_out[d.cols:2 * d.cols, :] = y1.T

        def body(q, x):
            for po, out in ((po0, p0_out), (po1, p1_out)):
                for t in range(2):
                    r = q * 2 + t
                    v = po[r].T
                    for h in range(d.halves):
                        for f in range(0, d.fields, 8):
                            at = h * d.fields + f
                            out[pl.ds(f * d.rows + h * d.r + r, 8, stride=d.rows), :] = v[at:at + 8]
            return x

        lax.fori_loop(0, d.r // 2, body, 0)

    scopies, total = all_sum(x_ref, sum_land, sum_s, sum_r, meanwhile)
    ym_out[2 * d.cols:2 * d.cols + 8, :] = jnp.broadcast_to(total, (8, LANES))
    for c in ecopies + gcopies + ycopies + zcopies + scopies:
        c.wait_send()


def final_kernel(d, steps, p0, p1, ym, c_ref, inc_ref, buf, sem):
    m = ym[2 * d.cols:2 * d.cols + 1]
    m = [m[:, k:k + 1] for k in range(4)]
    bn2 = m[0] + EPS
    c = (EPS - m[1]) / bn2
    alpha1 = (m[0] + m[1]) / bn2
    r2 = jnp.maximum((c * c * m[0] + 2.0 * c * m[1] + m[2]) / bn2, 0.0)
    rho = (c * c * m[1] + 2.0 * c * m[2] + m[3]) / bn2
    b2 = r2 + EPS
    alpha2 = (r2 + rho) / b2
    det = alpha1 * alpha2 - b2
    ca, cb = (alpha2 - c) / det, -1.0 / det
    scale = KAPPA ** SWEEPS
    full = lambda v: jnp.broadcast_to(v, (8, LANES))
    sa, sb, ya, yb = full(ca * scale), full(cb * scale), full(ca), full(cb)
    size = c_ref.shape[0] // steps

    def copy(j):
        at = pl.ds(pl.multiple_of(j * size, size), size)
        return pltpu.make_async_copy(buf.at[at], c_ref.at[at], sem.at[j])

    def chunk(j, x):
        def some(i, x):
            for t in range(16):
                at = pl.ds(pl.multiple_of(j * size + i * 128 + t * 8, 8), 8)
                buf[at, :] = sa * p0[at, :] + sb * p1[at, :]
            return x

        lax.fori_loop(0, size // 128, some, 0)
        copy(j).start()
        return x

    lax.fori_loop(0, steps, chunk, 0)
    for l in range(d.levels):
        for t in range(0, d.rows, 8):
            at = l * d.rows + t
            inc_ref[l, t:t + 8] = ya * ym[at:at + 8] + yb * ym[d.cols + at:d.cols + at + 8]
    for j in range(steps):
        copy(j).wait()


def on_device(ensemble, obs_cell, obs_level, innovation, obs_weight):
    members, levels, rows, cols = ensemble.shape
    d = Dims(members, levels, rows, cols)
    nx, ny = lax.axis_size("gx"), lax.axis_size("gy")
    vm = pl.BlockSpec(memory_space=pltpu.VMEM)
    hbm = pl.BlockSpec(memory_space=pltpu.HBM)
    dma = pltpu.SemaphoreType.DMA
    v = lambda *s: pltpu.VMEM(s, f32)
    flat = lambda a: a.reshape(1, -1)
    shape = lambda *s: jax.ShapeDtypeStruct(s, f32)
    scratch = [v(d.fields * (rows + 1), LANES)] + [v(d.size, LANES)] * 9
    scratch += [pltpu.VMEM((d.rr // 2, 256, 256), bf16), pltpu.VMEM((d.rr * LANES, LANES), bf16),
                pltpu.VMEM((d.st, d.rr * LANES), bf16), v(d.r, cols, LANES), v(d.r, cols, LANES)]
    scratch += [v(d.groups * 8, LANES), v(8, LANES), v(8, LANES)]
    side = d.r * 4
    scratch += [v(2, cols, LANES), v(2, cols, LANES), v(side, LANES), v(side, LANES)] * 2
    scratch += [v(16, LANES)] * 4 + [dma((8,)), dma((8,))]
    scratch += [v(d.st, LANES)] * 10
    scratch += exchange_buffers(2) + exchange_buffers(1) + exchange_buffers(1)
    n = nx * ny - 1
    obs = obs_cell.shape[-1]
    scratch += [v(1, LANES), v(n, 1, LANES), dma((n,)), dma((n,))]
    scratch += [pltpu.VMEM(ensemble.shape, bf16)] + [pltpu.VMEM((1, obs), jnp.int32)] * 2 + [v(1, obs)] * 2
    scratch += [dma((8,))]

    def main_entry(*refs):
        main_kernel(d, *refs)

    p0, p1, ym = pl.pallas_call(
        main_entry,
        out_shape=(shape(d.fields * rows, cols), shape(d.fields * rows, cols), shape(2 * cols + 8, LANES)),
        in_specs=[hbm] * 5,
        out_specs=(vm, vm, vm),
        scratch_shapes=scratch,
        compiler_params=pltpu.CompilerParams(collective_id=0, has_side_effects=True, vmem_limit_bytes=48000000),
    )(*[pltpu.with_memory_space_constraint(a, pltpu.HBM) for a in (
        ensemble, flat(obs_cell), flat(obs_level), flat(innovation), flat(obs_weight))])
    steps = 8

    def final_entry(*refs):
        final_kernel(d, steps, *refs)

    control, increment = pl.pallas_call(
        final_entry,
        out_shape=(shape(d.fields * rows, cols), shape(levels, rows, cols)),
        in_specs=[vm] * 3,
        out_specs=(hbm, vm),
        scratch_shapes=[v(d.fields * rows, cols), dma((steps,))],
        compiler_params=pltpu.CompilerParams(vmem_limit_bytes=8000000),
    )(p0, p1, ym)
    return (control.reshape(members, levels, rows, cols), increment)


def solution(mesh):
    return jax.shard_map(
        on_device,
        mesh=mesh,
        in_specs=(
            P(None, None, "gy", "gx"),
            P("gy", "gx", None),
            P("gy", "gx", None),
            P("gy", "gx", None),
            P("gy", "gx", None),
        ),
        out_specs=(P(None, None, "gy", "gx"), P(None, "gy", "gx")),
        check_vma=False,
    )
```

```python
import math
import jax
import jax.numpy as jnp
from jax import lax
from jax.experimental import pallas as pl
from jax.experimental.pallas import tpu as pltpu
from jax.sharding import PartitionSpec as P

SWEEPS = 4
KAPPA = 0.2
EPS = 1e-06
D = SWEEPS
BASE = 8
LANES = 128
SIDES = [(-1, 0), (1, 0), (0, -1), (0, 1), (-1, -1), (-1, 1), (1, -1), (1, 1)]
N_, S_, W_, E_, NW, NE, SW, SE = range(8)
BACK = [S_, N_, E_, W_, SE, SW, NE, NW]
MESH = pl.DeviceIdType.MESH
f32, bf16 = jnp.float32, jnp.bfloat16


class Dims:
    def __init__(self, members, levels, rows, cols):
        self.members, self.levels, self.rows, self.cols = members, levels, rows, cols
        self.fields = members * levels
        self.halves = LANES // self.fields
        assert self.halves == 2 and cols == LANES and levels * rows == LANES
        self.r = rows // self.halves
        self.rr = self.r + 2 * D
        self.groups = (cols + 2 * D) // 8
        self.st = -(-(cols + 2 * D) // 16) * 16
        self.size = BASE + self.rr * self.st + 8


def peer(dy, dx):
    ny, nx = lax.axis_size("gy"), lax.axis_size("gx")
    return {"gy": lax.rem(lax.axis_index("gy") + dy + ny, ny), "gx": lax.rem(lax.axis_index("gx") + dx + nx, nx)}


def others():
    ny, nx = lax.axis_size("gy"), lax.axis_size("gx")
    return [(dy, dx) for dy in range(ny) for dx in range(nx) if dy or dx]


def meet_signal():
    bar = pltpu.get_barrier_semaphore()
    for dy, dx in others():
        pl.semaphore_signal(bar, inc=1, device_id=peer(dy, dx), device_id_type=MESH)


def meet_wait():
    pl.semaphore_wait(pltpu.get_barrier_semaphore(), len(others()))


def present(n):
    dy, dx = SIDES[n]
    gy, gx = lax.axis_index("gy") + dy, lax.axis_index("gx") + dx
    ok = None
    for d, i, axis in ((dy, gy, "gy"), (dx, gx, "gx")):
        if d:
            t = (i >= 0) if d < 0 else (i < lax.axis_size(axis))
            ok = t if ok is None else ok & t
    return ok


class Side:
    def __init__(self, n, src, dst, ssem, rsem):
        dy, dx = SIDES[n]
        self.n = n
        self.copy = pltpu.make_async_remote_copy(src_ref=src, dst_ref=dst, send_sem=ssem.at[n], recv_sem=rsem.at[n],
                                                 device_id=peer(dy, dx), device_id_type=MESH)
        pl.when(present(n))(self.copy.start)

    def wait_recv(self):
        pl.when(present(BACK[self.n]))(self.copy.wait_recv)

    def wait_send(self):
        pl.when(present(self.n))(self.copy.wait_send)


def clear_absent(n, refs):
    @pl.when(jnp.logical_not(present(n)))
    def _():
        for ref in refs:
            ref[...] = jnp.zeros_like(ref)


def lane_iota(rows):
    return lax.broadcasted_iota(jnp.int32, (rows, LANES), 1)


def flip(x):
    return pltpu.roll(x, LANES // 2, 1)


def scatter(d, cell_ref, level_ref, inn_ref, wt_ref, go, do):
    cell = cell_ref[...]
    row = level_ref[...] * d.rows + cell // d.cols
    col = cell % d.cols
    n = cell.shape[1]
    hot = jnp.where(lax.broadcasted_iota(jnp.int32, (d.levels * d.rows, n), 0) == row, 1.0, 0.0).astype(bf16)
    at = lax.broadcasted_iota(jnp.int32, (d.cols, n), 0) == col
    wt = wt_ref[...]
    for ref, v in ((go, wt * inn_ref[...]), (do, wt)):
        hi = v.astype(bf16).astype(f32)
        total = None
        for part in (hi, v - hi):
            sel = jnp.where(at, part, 0.0).astype(bf16)
            term = lax.dot_general(sel, hot, (((1,), (1,)), ((), ())), preferred_element_type=f32)
            total = term if total is None else total + term
        ref[D:D + d.cols, :] = total
        ref[0:D, :] = jnp.zeros((D, LANES), f32)
        ref[D + d.cols:d.st, :] = jnp.zeros((d.st - D - d.cols, LANES), f32)


def row_masks(d, rows):
    rowl = lane_iota(rows) % d.rows
    return rowl < D, rowl >= d.rows - D, (rowl >= d.r - D) & (rowl < d.r + D)


def exchange_buffers(n):
    v = lambda *s: pltpu.VMEM((n,) + s, f32)
    one = [v(3, 8, LANES)] * 2 + [v(2, 8, LANES)] * 2 + [v(8, LANES)] * 4
    dma = pltpu.SemaphoreType.DMA
    return one + one + [dma((8,)), dma((8,))]


def exchange_pack(d, pairs, bufs):
    out = bufs[:8]
    lo, hi, mid = row_masks(d, 8)
    last = d.groups - 1
    at = lambda g: slice(g * 8, g * 8 + 8)
    for a, (yo, yr) in enumerate(pairs):
        packs = [[None] * 3, [None] * 3]
        for g in range(d.groups):
            own, ring = yo[at(g), :], yr[at(g), :]
            own = own + jnp.where(mid, ring, 0.0)
            yo[at(g), :] = own
            for k in range(2):
                v = jnp.where(lo, own if k == 0 else ring, jnp.where(hi, ring if k == 0 else own, 0.0))
                if g == 0:
                    out[NW + 2 * k][a] = v
                if g == last:
                    out[NE + 2 * k][a] = v
                v = pltpu.roll(v, D + 8 * (g % 8), 1)
                packs[k][g // 8] = v if packs[k][g // 8] is None else packs[k][g // 8] + v
            if g == 0 or g == last:
                m = out[W_ if g == 0 else E_]
                m[a, 0] = own
                m[a, 1] = ring
        for k in range(2):
            for j in range(3):
                out[k][a, j] = packs[k][j]


def exchange_send(bufs):
    out, land, ssem, rsem = bufs[:8], bufs[8:16], bufs[16], bufs[17]
    return [Side(n, out[n], land[BACK[n]], ssem, rsem) for n in range(len(SIDES))]


def exchange_start(d, pairs, bufs):
    exchange_pack(d, pairs, bufs)
    return exchange_send(bufs)


def exchange_finish(d, pairs, bufs, copies):
    land = bufs[8:16]
    lo, hi, mid = row_masks(d, 8)
    last = d.groups - 1
    at = lambda g: slice(g * 8, g * 8 + 8)
    for c in copies:
        c.wait_recv()
    for a, (yo, yr) in enumerate(pairs):
        for g in range(d.groups):
            own, ring = yo[at(g), :], yr[at(g), :]
            shift = (LANES - D - 8 * (g % 8)) % LANES
            north = pltpu.roll(land[N_][a, g // 8], shift, 1)
            south = pltpu.roll(land[S_][a, g // 8], shift, 1)
            if g == 0:
                north, south = north + land[NW][a], south + land[SW][a]
            if g == last:
                north, south = north + land[NE][a], south + land[SE][a]
            if g == 0 or g == last:
                m = land[W_ if g == 0 else E_]
                own, ring = own + m[a, 0], ring + m[a, 1]
            own = own + jnp.where(lo, north, jnp.where(hi, south, 0.0))
            ring = ring + jnp.where(hi, north, jnp.where(lo, south, 0.0))
            yo[at(g), :] = own
            yr[at(g), :] = jnp.where(mid, own, ring)


def build_selectors(d, sel, bsel):
    def code(x_iota, l_iota, shift):
        level = x_iota // d.rows
        half = l_iota // d.fields
        base = lax.rem(lax.rem(x_iota, d.rows) - d.r * half - shift + d.rows, d.rows)
        return jnp.where(lax.rem(l_iota, d.levels) == level, base, -1)

    a = lax.broadcasted_iota(jnp.int32, (LANES, LANES), 0)
    b = lax.broadcasted_iota(jnp.int32, (LANES, LANES), 1)
    for_sel = code(a, b, 0)
    for_bsel = code(b, a, lax.rem(a, d.fields) // (d.fields // 2))

    def fill(q, x):
        want = lax.rem(q * 2 - D + d.rows, d.rows)
        two = jnp.where(for_bsel == want, 1.0, 0.0).astype(bf16)
        for k in range(2):
            bsel[pl.ds(pl.multiple_of(q * 256 + k * LANES, LANES), LANES), :] = two
        for s in range(2):
            one = jnp.where(for_sel == want + s, 1.0, 0.0).astype(bf16)
            for k in range(2):
                sel[q, k * LANES:(k + 1) * LANES, s * LANES:(s + 1) * LANES] = one
        return x

    lax.fori_loop(0, d.rr // 2, fill, 0)


def split(x):
    hi = x.astype(bf16)
    return hi, (x - hi.astype(f32)).astype(bf16)


def wide(ref):
    hi, lo = split(ref[...])
    return jnp.concatenate([hi, lo], axis=1)


def expand(d, x, pairs, sel, et, u):
    n = d.groups * 8
    for q in pairs:
        g2 = jnp.dot(x, sel[q], preferred_element_type=f32)
        for s in range(2):
            at = BASE + (2 * q + s) * d.st
            u[at:at + n, :] = et[at:at + n, :] * g2[0:n, s * LANES:(s + 1) * LANES]


def expand_edges(d, x, pairs, sel, et, u):
    n = d.groups * 8
    x = jnp.concatenate([x[0:8], x[n - 8:n]], axis=0)
    for q in pairs:
        g2 = jnp.dot(x, sel[q], preferred_element_type=f32)
        for s in range(2):
            for k in range(2):
                at = BASE + (2 * q + s) * d.st + k * (n - 8)
                u[at:at + 8, :] = et[at:at + 8, :] * g2[k * 8:k * 8 + 8, s * LANES:(s + 1) * LANES]


def stencil(d, src, p, lo, hi, use):
    def ld(r, o):
        return src[pl.ds(p + (BASE + (r + D) * d.st + o), 8), :]

    n, c = ld(lo - 1, 0), ld(lo, 0)
    for r in range(lo, hi):
        s = ld(r + 1, 0)
        use(r, (n + s) + (c + (ld(r, -1) + ld(r, 1))))
        n, c = c, s


def spread(n, rows, body):
    k = min(n, 5, max(1, 80 // rows))

    def step(i, x):
        for t in range(k):
            body(i * k + t)
        return x

    if n > k:
        lax.fori_loop(0, n // k, step, 0)
        for t in range(n // k * k, n):
            body(t)
    else:
        for t in range(n):
            body(t)


def aligned(x, n):
    return x if isinstance(x, int) else pl.multiple_of(x, n)


def count(ranges):
    return sum(hi - lo for lo, hi in ranges)


def sweep_part(d, src, dst, ranges, groups, masks):
    def body(g):
        p = aligned(groups[0] * 8 + g * (groups[1] * 8), 8)
        if masks is not None:
            cm, rt, rb = masks
            m = cm[pl.ds(p, 8), :]
            mt, mb = m * rt[...], m * rb[...]

        def use(r, v):
            if masks is not None:
                v = v * (mt if r < 0 else mb if r >= d.r else m)
            dst[pl.ds(p + (BASE + (r + D) * d.st), 8), :] = v

        for lo, hi in ranges:
            stencil(d, src, p, lo, hi, use)

    spread(groups[2], count(ranges), body)


def last_part(d, src, pad, po, ranges, groups):
    def body(g):
        c = aligned(groups[0] * 8 + g * (groups[1] * 8), 8)

        def use(r, v):
            pad[pl.ds(c + (D + BASE + (r + D) * d.st), 8), :] = v
            po[r, pl.ds(c, 8), :] = v

        for lo, hi in ranges:
            stencil(d, src, c + D, lo, hi, use)

    spread(groups[2], count(ranges), body)


def filter_inner(d, src, bufs, pad, po, margin):
    groups = (0, 1, d.groups) if margin == 0 else (1, 1, d.groups - 2)
    for k, dst in enumerate(bufs):
        m = margin + k + 1
        sweep_part(d, src, dst, [(m, d.r - m)], groups, None)
        src = dst
    m = margin + SWEEPS
    last_part(d, src, pad, po, [(m, d.r - m)], (1, 1, d.cols // 8 - 2))


def filter_outer(d, src, bufs, pad, po, margin, masks):
    for k, dst in enumerate(bufs):
        m, e = margin + k + 1, SWEEPS - k - 1
        w = 2 if margin else 1
        sweep_part(d, src, dst, [(-e, m), (d.r - m, d.r + e)], (w, 1, d.groups - 2 * w), masks)
        for t in range(w):
            sweep_part(d, src, dst, [(-e, d.r + e)], (t, d.groups - w, 2), masks)
        src = dst
    m = margin + SWEEPS
    n = d.cols // 8
    last_part(d, src, pad, po, [(0, m), (d.r - m, d.r)], (1, 1, n - 2))
    last_part(d, src, pad, po, [(0, d.r)], (0, n - 1, 2))


def spread_back(d, src, et, lhs, p, both, ranges):
    first = lane_iota(8) % d.fields < d.fields // 2
    quarter = d.fields // 2
    keys = range(2 if both else 1)

    def ld(r, o):
        return src[pl.ds(p + (BASE + (r + D) * d.st + o), 8), :]

    for lo, hi in ranges:
        n = [ld(lo - 1, 8 * k) if lo > -D else None for k in keys]
        c = [ld(lo, 8 * k) for k in keys]
        even = None
        for r in range(lo, hi):
            ts = []
            for k in keys:
                o = 8 * k
                v = c[k] + (ld(r, o - 1) + ld(r, o + 1))
                s = None
                if r < d.r + D - 1:
                    s = ld(r + 1, o)
                    v = v + s
                if n[k] is not None:
                    v = v + n[k]
                n[k], c[k] = c[k], s
                ts.append(v * et[pl.ds(p + (BASE + (r + D) * d.st + o), 8), :])
            if (r + D) % 2 == 0:
                even = ts
                continue
            folded = [jnp.where(first, a, b) + jnp.where(first, pltpu.roll(a, LANES - quarter, 1), pltpu.roll(b, quarter, 1))
                      for a, b in zip(even, ts)]
            if not both:
                folded.append(jnp.zeros((8, LANES), f32))
            up, down = split(jnp.concatenate(folded, axis=0))
            at = (r + D) // 2 * 2 * LANES
            lhs[pl.ds(p, 16), at:at + LANES] = up
            lhs[pl.ds(p, 16), at + LANES:at + 2 * LANES] = down


def back_pairs(d, src, et, lhs, start, n, ranges):
    def body(g, x):
        spread_back(d, src, et, lhs, pl.multiple_of((start + g) * 16, 16), True, ranges)
        return x

    lax.fori_loop(0, n, body, 0)


def back_inner(d, pad, bufs, et, lhs):
    src = pad
    for k, dst in enumerate(bufs):
        m = D + k + 1
        sweep_part(d, src, dst, [(m, d.r - m)], (1, 1, d.groups - 2), None)
        src = dst
    back_pairs(d, src, et, lhs, 1, d.groups // 2 - 2, [(2 * D, d.r - 2 * D)])


def back_filter(d, pad, bufs, et, lhs, masks, inner_done):
    src = pad
    for k, dst in enumerate(bufs):
        e, m = k + 1, D + k + 1
        if inner_done:
            sweep_part(d, src, dst, [(-e, m), (d.r - m, d.r + e)], (2, 1, d.groups - 4), masks)
            for t in range(2):
                sweep_part(d, src, dst, [(-e, d.r + e)], (t, d.groups - 2, 2), masks)
        else:
            sweep_part(d, src, dst, [(-e, d.r + e)], (0, 1, d.groups), masks)
        src = dst
    rows = [(-D, d.r + D)]
    n = d.groups // 2
    if inner_done:
        back_pairs(d, src, et, lhs, 1, n - 2, [(-D, 2 * D), (d.r - 2 * D, d.r + D)])
        for q in (0, n - 1):
            spread_back(d, src, et, lhs, q * 16, True, rows)
    else:
        back_pairs(d, src, et, lhs, 0, n, rows)
    spread_back(d, src, et, lhs, n * 16, False, rows)


def reduce_members(d, lhs, bsel, yo, yr):
    k0, k1, k2 = D * LANES, (D + d.r) * LANES, d.rr * LANES
    scale = KAPPA ** (2 * SWEEPS)
    dot = lambda a, b: jnp.dot(lhs[:, a:b], bsel[a:b, :], preferred_element_type=f32)
    yo[...] = dot(k0, k1) * scale
    yr[...] = (dot(0, k0) + dot(k1, k2)) * scale


def all_sum(x_ref, land, ssem, rsem, meanwhile):
    copies = []
    for k, (dy, dx) in enumerate(others()):
        copies.append(pltpu.make_async_remote_copy(
            src_ref=x_ref, dst_ref=land.at[k], send_sem=ssem.at[k], recv_sem=rsem.at[k],
            device_id=peer(dy, dx), device_id_type=MESH))
        copies[-1].start()
    meanwhile()
    for c in copies:
        c.wait_recv()
    total = x_ref[...]
    for k in range(len(copies)):
        total = total + land[k]
    return copies, total


def ens_send_rows(d, et, hn, hs):
    lane = lane_iota(d.cols)
    low = lane < LANES // 2
    at = lambda r: et[BASE + (r + D) * d.st + D:BASE + (r + D) * d.st + D + d.cols, :]
    for i in range(2):
        hn[i] = jnp.where(low, at(i), flip(at(i + 2)))
        hs[i] = jnp.where(low, flip(at(d.r - 2 + i)), at(d.r - 4 + i))


def main_kernel(d, ens_in, cell_in, level_in, inn_in, wt_in, p0_out, p1_out, ym_out, *refs):
    refs = list(refs)
    take = lambda n: [refs.pop(0) for _ in range(n)]
    ec, et, u, a1, a2, a3, pad, b1, b2, b3 = take(10)
    sel, bsel, lhs, po0, po1 = take(5)
    cm, rt, rb = masks = take(3)
    hn, hs, hw, he, ln, ls, lw, le, lnw, lne, lsw, lse, esem, rsem = take(14)
    go, gr, do, dr, g1o, g1r, y0o, y0r, y1o, y1r = take(10)
    ex0, exd, ex1, ex2 = take(18), take(18), take(18), take(18)
    x_ref, sum_land, sum_s, sum_r = take(4)
    ens, cell, level, inn, wt, isem = take(6)
    es = d.rows + 1
    gy, gx = lax.axis_index("gy"), lax.axis_index("gx")
    ny, nx = lax.axis_size("gy"), lax.axis_size("gx")
    flag = lambda b: jnp.where(b, 1.0, 0.0).astype(f32)
    hasn, hass, hasw, hase = flag(gy > 0), flag(gy < ny - 1), flag(gx > 0), flag(gx < nx - 1)

    meet_signal()
    chunk = d.members // 4
    loads = [pltpu.make_async_copy(ens_in.at[pl.ds(k * chunk, chunk)], ens.at[pl.ds(k * chunk, chunk)], isem.at[k])
             for k in range(4)]
    small = [pltpu.make_async_copy(a, b, isem.at[4 + k])
             for k, (a, b) in enumerate(((cell_in, cell), (level_in, level), (inn_in, inn), (wt_in, wt)))]
    for c in small + loads:
        c.start()
    for n, refs_n in enumerate(((ln,), (ls,), (lw,), (le,), (lnw,), (lne,), (lsw,), (lse,))):
        clear_absent(n, refs_n + tuple(ex[8 + n] for ex in (ex0, exd, ex1, ex2)))
    for c in small:
        c.wait()
    scatter(d, cell, level, inn, wt, go, do)
    gr[...] = jnp.zeros_like(gr)
    dr[...] = jnp.zeros_like(dr)
    gpairs, dpairs = [(go, gr)], [(do, dr)]
    exchange_pack(d, gpairs, ex0)
    exchange_pack(d, dpairs, exd)

    def convert(k, x):
        for l in range(d.levels):
            ec[pl.ds((k * d.levels + l) * es, d.rows), :] = ens[k, l].astype(f32)
        return x

    for k in range(4):
        loads[k].wait()
        lax.fori_loop(k * chunk, (k + 1) * chunk, convert, 0)

    def transpose_row(r):
        parts = []
        for h in range(d.halves):
            for f in range(0, d.fields, 8):
                parts.append(ec[pl.ds(f * es + h * d.r + r, 8, stride=es), :])
        et[pl.ds(BASE + (r + D) * d.st + D, d.cols), :] = jnp.concatenate(parts, axis=0).T

    def transpose_four(q):
        for t in range(4):
            transpose_row(q * 4 + t)
        for t in range(4):
            r = q * 4 + t
            at = BASE + (r + D) * d.st + D
            to = pl.ds(pl.multiple_of(r * 4, 4), 4)
            hw[to, :] = et[pl.ds(at, 4), :]
            he[to, :] = et[pl.ds(at + d.cols - 4, 4), :]

    def transpose_edges(k, x):
        transpose_four(k * (d.r // 4 - 1))
        return x

    def transpose_two(k, x):
        transpose_four(k * 2 + 1)
        transpose_four(k * 2 + 2)
        return x

    lax.fori_loop(0, 2, transpose_edges, 0)
    ens_send_rows(d, et, hn, hs)
    n4 = d.r * 4
    meet_wait()
    gcopies = exchange_send(ex0)
    ecopies = [Side(N_, hn, ls, esem, rsem), Side(S_, hs, ln, esem, rsem)]
    lax.fori_loop(0, d.r // 8 - 1, transpose_two, 0)
    ecopies += [Side(W_, hw, le, esem, rsem), Side(E_, he, lw, esem, rsem),
                Side(NW, hw.at[0:16], lse, esem, rsem), Side(NE, he.at[0:16], lsw, esem, rsem),
                Side(SW, hw.at[n4 - 16:n4], lne, esem, rsem), Side(SE, he.at[n4 - 16:n4], lnw, esem, rsem)]
    dcopies = exchange_send(exd)
    build_selectors(d, sel, bsel)
    edge = D // 2
    pairs = d.rr // 2
    ring_pairs = lambda n: list(range(n)) + list(range(pairs - n, pairs))
    a_bufs = (a1, a2, a3)
    expand(d, wide(go), range(edge, pairs - edge), sel, et, u)
    filter_inner(d, u, a_bufs, pad, po0, 0)
    back_inner(d, pad, (b1, b2, b3), et, lhs)
    p = lax.broadcasted_iota(jnp.int32, (d.groups * 8, LANES), 0)
    cm[...] = jnp.where(p < D, hasw, jnp.where(p >= D + d.cols, hase, 1.0))
    low8 = lane_iota(8) < LANES // 2
    rt[...] = jnp.where(low8, hasn, 1.0)
    rb[...] = jnp.where(low8, 1.0, hass)

    zero = lambda n: jnp.zeros((n, LANES), f32)
    for ref, ext in ((pad, 0), (b1, 1), (b2, 2), (b3, 3)):
        for r in range(-min(ext + 2, D), d.r + min(ext + 2, D)):
            at = BASE + (r + D) * d.st
            if r < -ext or r >= d.r + ext:
                ref[at:at + d.st, :] = zero(d.st)
            else:
                ref[at + d.groups * 8:at + d.st, :] = zero(d.st - d.groups * 8)
                if ext == 0:
                    ref[at:at + D, :] = zero(D)
                    ref[at + D + d.cols:at + d.groups * 8, :] = zero(D)
        ref[0:BASE, :] = zero(BASE)
        ref[BASE + d.rr * d.st:d.size, :] = zero(8)

    exchange_finish(d, gpairs, ex0, gcopies)
    for c in ecopies:
        c.wait_recv()
    low = lane_iota(d.cols) < LANES // 2
    row_at = lambda r: BASE + (r + D) * d.st
    own = lambda r: et[row_at(r) + D:row_at(r) + D + d.cols, :]
    for j in range(D):
        south = ls[j % 2]
        north = ln[j % 2]
        if j < 2:
            sv = flip(jnp.where(low, south, own(j)))
            nv = flip(jnp.where(low, own(d.r - 4 + j), north))
        else:
            sv = jnp.where(low, flip(own(j)), south)
            nv = jnp.where(low, north, flip(own(d.r - 4 + j)))
        et[row_at(d.r + j) + D:row_at(d.r + j) + D + d.cols, :] = sv
        et[row_at(j - D) + D:row_at(j - D) + D + d.cols, :] = nv
    low16 = lane_iota(16) < LANES // 2
    for land, north, south, off in ((lw, lnw, lsw, 0), (le, lne, lse, D + d.cols)):
        for r in range(d.r):
            et[row_at(r) + off:row_at(r) + off + 4, :] = land[r * 4:r * 4 + 4, :]
        nv = flip(jnp.where(low16, land[n4 - 16:n4, :], north[...]))
        sv = flip(jnp.where(low16, south[...], land[0:16, :]))
        for j in range(D):
            et[row_at(j - D) + off:row_at(j - D) + off + 4, :] = nv[j * 4:j * 4 + 4, :]
            et[row_at(d.r + j) + off:row_at(d.r + j) + off + 4, :] = sv[j * 4:j * 4 + 4, :]

    def g_rest(g_o, g_r, po, yo, yr, margin):
        own, ring = wide(g_o), wide(g_r)
        expand(d, ring, ring_pairs(edge), sel, et, u)
        if margin:
            expand(d, own, list(range(edge, 2 * edge)) + list(range(pairs - 2 * edge, pairs - edge)), sel, et, u)
        first = edge + margin // 2
        expand_edges(d, own, range(first, pairs - first), sel, et, u)
        filter_outer(d, u, a_bufs, pad, po, margin, masks)
        back_filter(d, pad, (b1, b2, b3), et, lhs, masks, margin == 0)
        reduce_members(d, lhs, bsel, yo, yr)

    g_rest(go, gr, po0, y0o, y0r, 0)
    ycopies = exchange_start(d, [(y0o, y0r)], ex1)
    g1o[...] = do[...] * y0o[...]
    expand(d, wide(g1o), range(2 * edge, pairs - 2 * edge), sel, et, u)
    filter_inner(d, u, a_bufs, pad, po1, D)
    exchange_finish(d, dpairs, exd, dcopies)
    exchange_finish(d, [(y0o, y0r)], ex1, ycopies)
    g1o[...] = do[...] * y0o[...]
    g1r[...] = dr[...] * y0r[...]
    g_rest(g1o, g1r, po1, y1o, y1r, D)
    zcopies = exchange_start(d, [(y1o, y1r)], ex2)
    exchange_finish(d, [(y1o, y1r)], ex2, zcopies)
    inner = slice(D, D + d.cols)
    y0, y1, g0, g1, dd = y0o[inner, :], y1o[inner, :], go[inner, :], g1o[inner, :], do[inner, :]
    lane1 = lane_iota(1)
    x = jnp.zeros((1, LANES), f32)
    for k, v in enumerate((g0 * y0, g1 * y0, g1 * y1, dd * y1 * y1)):
        t = jnp.sum(jnp.sum(v, axis=0, keepdims=True), axis=1, keepdims=True)
        x = jnp.where(lane1 == k, t, x)
    x_ref[...] = x

    def meanwhile():
        ym_out[0:d.cols, :] = y0.T
        ym_out[d.cols:2 * d.cols, :] = y1.T

        def body(q, x):
            for po, out in ((po0, p0_out), (po1, p1_out)):
                for t in range(2):
                    r = q * 2 + t
                    v = po[r].T
                    for h in range(d.halves):
                        for f in range(0, d.fields, 8):
                            at = h * d.fields + f
                            out[pl.ds(f * d.rows + h * d.r + r, 8, stride=d.rows), :] = v[at:at + 8]
            return x

        lax.fori_loop(0, d.r // 2, body, 0)

    scopies, total = all_sum(x_ref, sum_land, sum_s, sum_r, meanwhile)
    ym_out[2 * d.cols:2 * d.cols + 8, :] = jnp.broadcast_to(total, (8, LANES))
    for c in ecopies + gcopies + dcopies + ycopies + zcopies + scopies:
        c.wait_send()


def final_kernel(d, steps, p0, p1, ym, c_ref, inc_ref, buf, sem):
    m = ym[2 * d.cols:2 * d.cols + 1]
    m = [m[:, k:k + 1] for k in range(4)]
    bn2 = m[0] + EPS
    c = (EPS - m[1]) / bn2
    alpha1 = (m[0] + m[1]) / bn2
    r2 = jnp.maximum((c * c * m[0] + 2.0 * c * m[1] + m[2]) / bn2, 0.0)
    rho = (c * c * m[1] + 2.0 * c * m[2] + m[3]) / bn2
    b2 = r2 + EPS
    alpha2 = (r2 + rho) / b2
    det = alpha1 * alpha2 - b2
    ca, cb = (alpha2 - c) / det, -1.0 / det
    scale = KAPPA ** SWEEPS
    full = lambda v: jnp.broadcast_to(v, (8, LANES))
    sa, sb, ya, yb = full(ca * scale), full(cb * scale), full(ca), full(cb)
    size = c_ref.shape[0] // steps

    def copy(j):
        at = pl.ds(pl.multiple_of(j * size, size), size)
        return pltpu.make_async_copy(buf.at[at], c_ref.at[at], sem.at[j])

    def chunk(j, x):
        def some(i, x):
            for t in range(16):
                at = pl.ds(pl.multiple_of(j * size + i * 128 + t * 8, 8), 8)
                buf[at, :] = sa * p0[at, :] + sb * p1[at, :]
            return x

        lax.fori_loop(0, size // 128, some, 0)
        copy(j).start()
        return x

    lax.fori_loop(0, steps, chunk, 0)
    for l in range(d.levels):
        for t in range(0, d.rows, 8):
            at = l * d.rows + t
            inc_ref[l, t:t + 8] = ya * ym[at:at + 8] + yb * ym[d.cols + at:d.cols + at + 8]
    for j in range(steps):
        copy(j).wait()


def on_device(ensemble, obs_cell, obs_level, innovation, obs_weight):
    members, levels, rows, cols = ensemble.shape
    d = Dims(members, levels, rows, cols)
    nx, ny = lax.axis_size("gx"), lax.axis_size("gy")
    vm = pl.BlockSpec(memory_space=pltpu.VMEM)
    hbm = pl.BlockSpec(memory_space=pltpu.HBM)
    dma = pltpu.SemaphoreType.DMA
    v = lambda *s: pltpu.VMEM(s, f32)
    flat = lambda a: a.reshape(1, -1)
    shape = lambda *s: jax.ShapeDtypeStruct(s, f32)
    scratch = [v(d.fields * (rows + 1), LANES)] + [v(d.size, LANES)] * 9
    scratch += [pltpu.VMEM((d.rr // 2, 256, 256), bf16), pltpu.VMEM((d.rr * LANES, LANES), bf16),
                pltpu.VMEM((d.st, d.rr * LANES), bf16), v(d.r, cols, LANES), v(d.r, cols, LANES)]
    scratch += [v(d.groups * 8, LANES), v(8, LANES), v(8, LANES)]
    side = d.r * 4
    scratch += [v(2, cols, LANES), v(2, cols, LANES), v(side, LANES), v(side, LANES)] * 2
    scratch += [v(16, LANES)] * 4 + [dma((8,)), dma((8,))]
    scratch += [v(d.st, LANES)] * 10
    scratch += exchange_buffers(1) * 4
    n = nx * ny - 1
    obs = obs_cell.shape[-1]
    scratch += [v(1, LANES), v(n, 1, LANES), dma((n,)), dma((n,))]
    scratch += [pltpu.VMEM(ensemble.shape, bf16)] + [pltpu.VMEM((1, obs), jnp.int32)] * 2 + [v(1, obs)] * 2
    scratch += [dma((8,))]

    def main_entry(*refs):
        main_kernel(d, *refs)

    p0, p1, ym = pl.pallas_call(
        main_entry,
        out_shape=(shape(d.fields * rows, cols), shape(d.fields * rows, cols), shape(2 * cols + 8, LANES)),
        in_specs=[hbm] * 5,
        out_specs=(vm, vm, vm),
        scratch_shapes=scratch,
        compiler_params=pltpu.CompilerParams(collective_id=0, has_side_effects=True, vmem_limit_bytes=48000000),
    )(*[pltpu.with_memory_space_constraint(a, pltpu.HBM) for a in (
        ensemble, flat(obs_cell), flat(obs_level), flat(innovation), flat(obs_weight))])
    steps = 8

    def final_entry(*refs):
        final_kernel(d, steps, *refs)

    control, increment = pl.pallas_call(
        final_entry,
        out_shape=(shape(d.fields * rows, cols), shape(levels, rows, cols)),
        in_specs=[vm] * 3,
        out_specs=(hbm, vm),
        scratch_shapes=[v(d.fields * rows, cols), dma((steps,))],
        compiler_params=pltpu.CompilerParams(vmem_limit_bytes=8000000),
    )(p0, p1, ym)
    return (control.reshape(members, levels, rows, cols), increment)


def solution(mesh):
    return jax.shard_map(
        on_device,
        mesh=mesh,
        in_specs=(
            P(None, None, "gy", "gx"),
            P("gy", "gx", None),
            P("gy", "gx", None),
            P("gy", "gx", None),
            P("gy", "gx", None),
        ),
        out_specs=(P(None, None, "gy", "gx"), P(None, "gy", "gx")),
        check_vma=False,
    )
```
